32 devices in a mesh: slab: 16 (over z, y, x), feat: 2 (over core).
Axes of the slice: x: 2, y: 2, z: 4, core: 2. Of those that a mesh axis runs over, the one named last changes fastest.
Arguments:
- states: float32 [40, 8192], P(None, ('slab', 'feat')), may hold values from -6 to 6
- inputs: float32 [8192], P(('slab', 'feat')), may hold values from -4 to 4
- targets: float32 [40, 8192], P(None, ('slab', 'feat')), may hold values from -4 to 4
Outputs:
- local_operators: float32 [16, 40, 862], P('slab', 'feat')
- scaled_duals: float32 [16, 40, 862], P('slab', 'feat')
- consensus: float32 [40, 862], P('feat')
- residual_history: float32 [2, 2], replicated
The draws below stay inside these ranges and needn't reach their ends.
All inputs are finite; a program needn't handle non-finite values.
Results may differ from the reference program's by a relative error of at most 0.0003.
Values sent between devices are 32-bit elements; how exact they have to be, the bound alone decides.
A program may use at most 64 MiB of HBM per device.

```python
import jax
import jax.numpy as jnp
from jax import lax

R = 40
ITERS = 2
FEATS = 862
SNAPS = 8192
N_SLAB = 16


def joint_draw(key):
    folded = jax.random.fold_in(key, 9031)
    streams = jax.random.split(folded, 10)
    slab_rows = SNAPS // N_SLAB
    slab_scale = jax.random.uniform(streams[0], (N_SLAB,), minval=0.7, maxval=1.4)
    unit_draw = jnp.clip(jax.random.normal(streams[1], (R, N_SLAB, slab_rows)), -4.0, 4.0)
    states = unit_draw * slab_scale[None, :, None]
    forcing = jnp.clip(jax.random.normal(streams[2], (N_SLAB, slab_rows)), -4.0, 4.0)
    root = R ** 0.5
    linear = jax.random.normal(streams[3], (R, R)) / root
    slab_drift = 0.6 * jax.random.normal(streams[4], (N_SLAB, R, R)) / root
    square_map = 0.3 * jax.random.normal(streams[5], (R, R)) / root
    mixed_map = 0.3 * jax.random.normal(streams[6], (R, R)) / root
    input_gain = jax.random.normal(streams[7], (R,))
    offset = jax.random.normal(streams[8], (R,))
    noise_part = 0.3 * jax.random.normal(streams[9], (R, N_SLAB, slab_rows))
    signal = jnp.einsum('ij,jsk->isk', linear, states)
    signal = signal + jnp.einsum('sij,jsk->isk', slab_drift, states)
    signal = signal + jnp.einsum('ij,jsk->isk', square_map, states * states)
    signal = signal + jnp.einsum('ij,jsk->isk', mixed_map, states * jnp.roll(states, 1, axis=0))
    signal = signal + input_gain[:, None, None] * forcing[None] + offset[:, None, None] + noise_part
    targets = 4.0 * jnp.tanh(signal / 4.0)
    return (states.reshape(R, SNAPS), forcing.reshape(SNAPS), targets.reshape(R, SNAPS))


def draw_states(key, part):
    return joint_draw(key)[0].astype(jnp.float32)


def draw_inputs(key, part):
    return joint_draw(key)[1].astype(jnp.float32)


def draw_targets(key, part):
    return joint_draw(key)[2].astype(jnp.float32)


def setup_inputs(seed: int = 0) -> dict:
    streams_of = jax.random.split(jax.random.key(seed), 4)
    return {
        "states": draw_states(jax.random.fold_in(streams_of[3], 71), 0),
        "inputs": draw_inputs(jax.random.fold_in(streams_of[3], 71), 0),
        "targets": draw_targets(jax.random.fold_in(streams_of[3], 71), 0),
    }


penalty = 1.0

def features(states, inputs):
    reduced = states.shape[0]
    blocks = [states]
    for column in range(reduced):
        blocks.append(states[column:column + 1] * states[column:])
    blocks.append(inputs[None, :])
    blocks.append(jnp.ones_like(inputs)[None, :])
    return jnp.concatenate(blocks, 0)

def reference(states, inputs, targets):
    reduced = states.shape[0]
    slab_rows = states.shape[1] // N_SLAB
    slab_states = states.reshape(reduced, N_SLAB, slab_rows).transpose(1, 0, 2)
    slab_targets = targets.reshape(reduced, N_SLAB, slab_rows).transpose(1, 0, 2)
    slab_inputs = inputs.reshape(N_SLAB, slab_rows)

    def local_solve(packed):
        part_states, part_inputs, part_targets, shifted = packed
        design = features(part_states, part_inputs)
        gram_matrix = jnp.dot(design.astype(jnp.float32), design.T.astype(jnp.float32), precision=lax.Precision.HIGHEST, preferred_element_type=jnp.float32) / slab_rows
        cross = jnp.dot(part_targets.astype(jnp.float32), design.T.astype(jnp.float32), precision=lax.Precision.HIGHEST, preferred_element_type=jnp.float32) / slab_rows
        system = gram_matrix + penalty * jnp.eye(design.shape[0], dtype=jnp.float32)
        return jnp.linalg.solve(system, (cross + penalty * shifted).T).T
    width = FEATS
    consensus = jnp.zeros((reduced, width), jnp.float32)
    duals = jnp.zeros((N_SLAB, reduced, width), jnp.float32)
    primal_list = []
    dual_list = []
    operators = duals
    for sweep in range(ITERS):
        operators = lax.map(local_solve, (slab_states, slab_inputs, slab_targets, consensus[None] - duals))
        updated = lax.optimization_barrier(jnp.sum(operators + duals, 0)) / N_SLAB
        duals = duals + operators - updated[None]
        primal_list.append(jnp.sum(jnp.square(operators - updated[None])))
        dual_list.append(N_SLAB * penalty * penalty * jnp.sum(jnp.square(updated - consensus)))
        consensus = updated
    history = jnp.stack([jnp.stack(primal_list), jnp.stack(dual_list)])
    return (operators, duals, consensus, jnp.sqrt(history / (N_SLAB * reduced * width)))
```

```python
import functools

import jax
import jax.numpy as jnp
from jax import lax
from jax.experimental import pallas as pl
from jax.experimental.pallas import tpu as pltpu
from jax.sharding import PartitionSpec as P

penalty = 1.0
LIMIT = 20 * 2**20
LANES = 128
NN = (((1,), (0,)), ((), ()))
NT = (((1,), (1,)), ((), ()))
TN = (((0,), (0,)), ((), ()))
F32 = jnp.float32
BF16 = jnp.bfloat16


def up(value, step):
    return -(-value // step) * step


def dot(left, right, dims=NN):
    return lax.dot_general(left.astype(BF16), right.astype(BF16), dims, preferred_element_type=F32)


def split(value):
    high = value.astype(BF16)
    return high, (value - high.astype(F32)).astype(BF16)


def thin(left, high, low, dims=NN):
    rows = left.shape[0]
    top = left.astype(BF16).astype(F32)
    both = jnp.concatenate([top, left - top], 0).astype(BF16)
    out = dot(both, high, dims) + dot(both, low, dims)
    return out[:rows] + out[rows:]


def eye_mask(size):
    return lax.broadcasted_iota(jnp.int32, (size, size), 0) == lax.broadcasted_iota(jnp.int32, (size, size), 1)


def eye(size):
    return jnp.where(eye_mask(size), 1.0, 0.0)


def invert_by_pivots(source, target):
    size = source.shape[0]
    target[...] = source[...]
    sub = lax.broadcasted_iota(jnp.int32, (size, 1), 0)
    lane = lax.broadcasted_iota(jnp.int32, (1, size), 1)

    def step(k, carry):
        row = target[pl.ds(k, 1), :]
        here = lane == k
        pivot = jnp.sum(jnp.where(here, row, 0.0), axis=1, keepdims=True)
        scaled = jnp.where(here, 1.0, row) / pivot
        whole = target[...]
        column = jnp.sum(jnp.where(here, whole, 0.0), axis=1, keepdims=True)
        column = jnp.where(sub == k, -1.0, column)
        kept = jnp.where(here | (sub == k), 0.0, whole)
        target[...] = kept - column * scaled
        return carry

    lax.fori_loop(0, size, step, 0)


def exchange_kernel(states, inputs, targets, packed, far_s, far_u, far_t, send, recv):
    feats = lax.axis_size("feat")
    core = lax.axis_index("feat")
    reduced, own = states.shape
    half = reduced // feats
    scale = 1.0 / (own * feats)

    def moves(f):
        peer = lax.rem(core + f, feats)
        pairs = ((states, far_s), (inputs, far_u), (targets, far_t))
        return [
            pltpu.make_async_remote_copy(
                src_ref=source, dst_ref=target.at[f - 1], send_sem=send.at[f - 1, i], recv_sem=recv.at[f - 1, i],
                device_id={"feat": peer}, device_id_type=pl.DeviceIdType.MESH,
            )
            for i, (source, target) in enumerate(pairs)
        ]

    def place(f, s, u, t):
        spot = slice(f * own, (f + 1) * own)
        packed[0:reduced, spot] = s[...]
        packed[packed.shape[0] - 1 :, spot] = u[...]
        for c in range(feats):

            @pl.when(core == c)
            def _():
                packed[reduced : reduced + half, spot] = t[c * half : (c + 1) * half, :] * scale

    barrier = pltpu.get_barrier_semaphore()
    for f in range(1, feats):
        pl.semaphore_signal(
            barrier, inc=1, device_id={"feat": lax.rem(core + f, feats)}, device_id_type=pl.DeviceIdType.MESH
        )
    pl.semaphore_wait(barrier, feats - 1)
    for f in range(1, feats):
        for move in moves(f):
            move.start()
    rest = packed.shape[0] - 1 - reduced - half
    packed[reduced + half : reduced + half + rest, :] = jnp.zeros((rest, packed.shape[1]), F32)
    place(0, states, inputs, targets)
    for f in range(1, feats):
        for move in moves(f):
            move.wait_recv()
        place(f, far_s.at[f - 1], far_u.at[f - 1], far_t.at[f - 1])
    for f in range(1, feats):
        for move in moves(f):
            move.wait_send()


def stacked_gram(value, orders):
    parts = []
    rest = value
    for _ in range(1 + max(max(order) for order in orders)):
        high = rest.astype(BF16).astype(F32)
        parts.append(high)
        rest = rest - high
    left = jnp.concatenate([parts[i] for i, _ in orders], 0)
    right = jnp.concatenate([parts[j] for _, j in orders], 0)
    return dot(left, right, TN)


def inverse_kernel(packed, high_a, low_a, inverse, high_x, low_x, y, r, system, shifted, *, reduced, half):
    count = packed.shape[1]
    rows = y.shape[0]
    s = packed[0:reduced, :]
    signal = packed[packed.shape[0] - 1 :, :]
    inner = stacked_gram(s, ((0, 0), (0, 1), (1, 0), (0, 2), (2, 0), (1, 1)))
    extra = jnp.concatenate([s * s * (0.5**0.5), jnp.broadcast_to(signal, (8, count)) * (8.0**-0.5)], 0)
    a = inner + 0.5 * inner * inner + stacked_gram(extra, ((0, 0), (0, 1), (1, 0))) + 1.0
    a = a * (1.0 / count) + jnp.where(eye_mask(count), penalty, 0.0)
    system[...] = a
    high_a[...], low_a[...] = split(a)

    high = jnp.max(jnp.sum(jnp.abs(a), axis=0, keepdims=True)) / penalty
    delta = (high - 1.0) / (high + 1.0)
    alpha = 2.0 / ((1.0 + high) * penalty)
    c = 2.0 / (2.0 - delta * delta)
    inverse[...] = (c * alpha) * (jnp.where(eye_mask(count), 2.0, 0.0) - alpha * a)
    delta = delta * delta / (2.0 - delta * delta)

    def coarse(state):
        step, delta = state
        x = inverse[...].astype(BF16)
        shifted[...] = dot(high_a[...], x).astype(BF16)
        c = 2.0 / (2.0 - delta * delta)
        inverse[...] = c * (2.0 * inverse[...] - dot(x, shifted[...]))
        return step + 1, delta * delta / (2.0 - delta * delta)

    lax.while_loop(lambda state: (state[1] > 0.1) & (state[0] < 12), coarse, (0, delta))

    sub = lax.broadcasted_iota(jnp.int32, (rows, count), 0)
    mixed = (lax.broadcasted_iota(jnp.int32, (rows, count), 1) + 1) * (sub * 40503 + 30011)
    mixed = (mixed ^ (mixed >> 7)) * 9973
    signs = jnp.where(((mixed >> 9) & 1) == 1, 1.0, -1.0)
    b = jnp.where(sub < half, packed[reduced : reduced + rows, :], signs)

    def solve():
        high_x[...], low_x[...] = split(inverse[...])
        first = thin(b, high_x[...], low_x[...])
        left = b - thin(first, high_a[...], low_a[...])
        y[...] = first
        r[...] = left
        return jnp.sum(jnp.where(sub < half, 0.0, left * left)) * (1.0 / (rows - half))

    x = inverse[...].astype(BF16)
    shifted[...] = (eye(count) - (dot(high_a[...], x) + dot(low_a[...], x))).astype(BF16)
    inverse[...] = x.astype(F32) + dot(x, shifted[...])

    def polish(state):
        step, _ = state
        xh, xl = high_x[...], low_x[...]
        gap = eye(count) - (dot(high_a[...], xh) + (dot(high_a[...], xl) + dot(low_a[...], xh)))
        shifted[...] = gap.astype(BF16)
        inverse[...] = inverse[...] + dot(xh, shifted[...])
        return step + 1, solve()

    _, worst = lax.while_loop(
        lambda state: jnp.logical_not(state[1] < 0.01) & (state[0] < 6), polish, (0, solve())
    )

    @pl.when(jnp.logical_not(worst < 0.01))
    def _():
        invert_by_pivots(system, inverse)
        solve()


def build_features(packed, phi, reduced):
    count = packed.shape[1]
    row = reduced
    phi[0:reduced, :] = packed[0:reduced, :]
    for i in range(reduced):
        phi[row : row + reduced - i, :] = packed[i : i + 1, :] * packed[i:reduced, :]
        row += reduced - i
    phi[row : row + 1, :] = packed[packed.shape[0] - 1 :, :]
    phi[row + 1 : row + 2, :] = jnp.ones((1, count), F32)
    if row + 2 < phi.shape[0]:
        phi[row + 2 :, :] = jnp.zeros((phi.shape[0] - row - 2, count), F32)


def total(value):
    flat = value.reshape(-1, value.shape[-1])
    return jnp.sum(jnp.sum(flat, axis=0, keepdims=True), axis=1, keepdims=True)


def second_kernel(
    packed, high_a, low_a, inverse, high_x, low_x, y, r, after, duals, last, history,
    phi, high_p, low_p, high_w, low_w, better, high_b, low_b, gap,
    own1, own2, land1, land2, out1, out2, mean1, mean2,
    send1, recv1, spread1, got1, send2, recv2, spread2, got2,
    *, reduced, half, width,
):
    slabs = lax.axis_size("slab")
    feats = lax.axis_size("feat")
    me = lax.axis_index("slab")
    core = lax.axis_index("feat")
    owners, _, wide = own1.shape
    base = (slabs - owners) // 2
    head = feats - 1
    rows, count = y.shape
    spot = jnp.clip(me - base, 0, owners - 1)
    owning = (core == head) & (me >= base) & (me < base + owners)

    def copy(source, target, send, recv, slab, feat):
        return pltpu.make_async_remote_copy(
            src_ref=source, dst_ref=target, send_sem=send, recv_sem=recv,
            device_id={"slab": slab, "feat": feat}, device_id_type=pl.DeviceIdType.MESH,
        )

    def each(first, stop, body):
        if stop - first <= 16:
            for d in range(first, stop):
                body(d)
            return

        def step(d, carry):
            body(d)
            return carry

        lax.fori_loop(first, stop, step, 0)

    def everyone(body):
        for f in range(feats):

            def one(d, f=f):
                body(lax.rem(me + d, slabs), lax.rem(core + f, feats), f, d)

            each(1 if f == 0 else 0, slabs, one)

    barrier = pltpu.get_barrier_semaphore()

    def greet(slab, feat):
        pl.semaphore_signal(
            barrier, inc=1, device_id={"slab": slab, "feat": feat}, device_id_type=pl.DeviceIdType.MESH
        )

    @pl.when(owning)
    def _():
        everyone(lambda slab, feat, f, d: greet(slab, feat))

    @pl.when(jnp.logical_not(owning))
    def _():
        each(0, owners, lambda k: greet(base + k, head))

    b = packed[reduced : reduced + rows, :]
    ah, al, xh, xl = high_a[...], low_a[...], high_x[...], low_x[...]
    answer = y[...] + thin(r[...], xh, xl)
    real = lax.broadcasted_iota(jnp.int32, (rows, 1), 0) < half
    build_features(packed, phi, reduced)
    high_p[...], low_p[...] = split(phi[...])
    left = jnp.where(real, b - thin(answer, ah, al), 0.0)
    answer = answer + thin(left, xh, xl)
    start_value = thin(answer, high_p[...], low_p[...], NT)
    for k in range(owners):
        own1[k] = start_value[:half, k * wide : (k + 1) * wide]

    @pl.when(owning)
    def _():
        pl.semaphore_wait(barrier, slabs * feats - 1)

    @pl.when(jnp.logical_not(owning))
    def _():
        pl.semaphore_wait(barrier, owners)

    def other(k):
        return jnp.logical_not((core == head) & (me == base + k))

    def scatter(source, landing, send, recv):
        def piece(k):
            return copy(source.at[k], landing.at[core, me], send.at[k], recv.at[core, me], base + k, head)

        def start(k):
            @pl.when(other(k))
            def _():
                piece(k).start()

        def finish(k):
            @pl.when(other(k))
            def _():
                piece(k).wait_send()

        each(0, owners, start)
        return finish

    def arrivals(source, landing, send, recv):
        landing[head, me] = source[spot]

        def wait(slab, feat, f, d):
            copy(source.at[0], landing.at[feat, slab], send.at[0], recv.at[feat, slab], me, core).wait_recv()

        everyone(wait)

    def spread(source, target, send, recv, wait=False):
        def one(slab, feat, f, d):
            move = copy(source.at[feat], target.at[spot], send.at[feat, slab], recv.at[spot], slab, feat)
            if wait:
                move.wait_send()
            else:
                move.start()

        everyone(one)

    def collected(source, target, send, recv):
        def wait(k):
            @pl.when(other(k))
            def _():
                copy(source.at[0], target.at[k], send.at[0, 0], recv.at[k], me, core).wait_recv()

        each(0, owners, wait)

    end1 = scatter(own1, land1, send1, recv1)

    gap[...] = (eye(count) - (dot(ah, xh) + (dot(ah, xl) + dot(al, xh)))).astype(BF16)
    better[...] = inverse[...] + dot(xh, gap[...])
    high_b[...], low_b[...] = split(better[...])
    bh, bl = high_b[...], low_b[...]
    gap[...] = (eye(count) - (dot(ah, bh) + (dot(ah, bl) + dot(al, bh)))).astype(BF16)
    better[...] = better[...] + dot(bh, gap[...])
    high_b[...], low_b[...] = split(better[...])

    @pl.when(owning)
    def _():
        arrivals(own1, land1, send1, recv1)
        for f in range(feats):
            out1[f] = land1[f].sum(0) * (1.0 / slabs)
        spread(out1, mean1, spread1, got1)
        mean1[spot] = out1[head]

    weights = dot(high_b[...], high_p[...], NT) + (
        dot(high_b[...], low_p[...], NT) + dot(low_b[...], high_p[...], NT)
    )
    high_w[...], low_w[...] = split(weights)
    collected(out1, mean1, spread1, got1)

    def joined(buffer):
        whole = jnp.concatenate([buffer[k][:half] for k in range(owners)], 1)
        return jnp.concatenate([whole, jnp.zeros((rows - half, whole.shape[1]), F32)], 0)

    first = joined(own1)
    mean = joined(mean1)
    v = thin(mean, high_p[...], low_p[...]) * (2.0 / (count * penalty)) + answer
    result = first + 2.0 * mean - thin(v, high_w[...], low_w[...])
    for k in range(owners):
        own2[k] = result[:half, k * wide : (k + 1) * wide]
    end2 = scatter(own2, land2, send2, recv2)
    after[...] = result

    @pl.when(owning)
    def _():
        primal1 = jnp.zeros((1, 1), F32)
        dual1 = jnp.zeros((1, 1), F32)
        for f in range(feats):
            primal1 = primal1 + total(jnp.square(land1[f] - out1[f][None]))
            dual1 = dual1 + total(jnp.square(out1[f]))
        arrivals(own2, land2, send2, recv2)
        primal2 = jnp.zeros((1, 1), F32)
        dual2 = jnp.zeros((1, 1), F32)
        for f in range(feats):
            new = land2[f].sum(0) * (1.0 / slabs)
            out2[f, 0:half] = new
            primal2 = primal2 + total(jnp.square(land2[f] - new[None]))
            dual2 = dual2 + total(jnp.square(new - out1[f]))
        scale = slabs * penalty * penalty
        lane = lax.broadcasted_iota(jnp.int32, (1, wide), 1)
        sums = jnp.where(lane == 0, primal1, jnp.where(lane == 1, primal2, 0.0))
        sums = jnp.where(lane == 2, dual1 * scale, jnp.where(lane == 3, dual2 * scale, sums))
        for f in range(feats):
            out2[f, half : half + 1] = sums
        spread(out2, mean2, spread2, got2)
        mean2[spot] = out2[head]

    each(0, owners, end1)
    each(0, owners, end2)

    @pl.when(owning)
    def _():
        spread(out1, mean1, spread1, got1, wait=True)

    collected(out2, mean2, spread2, got2)
    new = joined(mean2)
    last[...] = new
    duals[...] = (first - mean) + (result - new)
    sums = mean2[0][half : half + 1]
    for k in range(1, owners):
        sums = sums + mean2[k][half : half + 1]
    roots = jnp.sqrt(sums[:, 0:LANES] * (1.0 / (slabs * reduced * width)))
    history[...] = jnp.broadcast_to(roots, history.shape)

    @pl.when(owning)
    def _():
        spread(out2, mean2, spread2, got2, wait=True)


def last_kernel(after, duals, last, history, out_after, out_duals, out_last, out_history):
    half, width = out_last.shape
    for r in range(half):
        out_after[r] = after[r : r + 1, :width]
        out_duals[r] = duals[r : r + 1, :width]
    out_last[...] = last[:half, :width]
    out_history[0:1, :] = history[0:1, 0:2]
    out_history[1:2, :] = history[0:1, 2:4]


def shards(states, inputs, targets):
    reduced, own = states.shape
    feats = lax.axis_size("feat")
    slabs = lax.axis_size("slab")
    half = reduced // feats
    width = reduced + reduced * (reduced + 1) // 2 + 2
    count = own * feats
    rows = up(half + 1, 8)
    tiles = up(width, LANES) // LANES
    wide = -(-tiles // slabs) * LANES
    columns = up(width, wide)
    owners = columns // wide
    vmem = pl.BlockSpec(memory_space=pltpu.VMEM)
    dma = pltpu.SemaphoreType.DMA

    def shape(*sizes, dtype=F32):
        return jax.ShapeDtypeStruct(sizes, dtype)

    def hold(*sizes, dtype=F32):
        return pltpu.VMEM(sizes, dtype)

    others = max(feats - 1, 1)
    packed = pl.pallas_call(
        exchange_kernel,
        out_shape=shape(reduced + rows + 1, count),
        in_specs=[vmem] * 3,
        out_specs=vmem,
        scratch_shapes=[
            hold(others, reduced, own), hold(others, 1, own), hold(others, reduced, own),
            dma((others, 3)), dma((others, 3)),
        ],
        compiler_params=pltpu.CompilerParams(vmem_limit_bytes=LIMIT, collective_id=1, has_side_effects=True),
        name="exchange",
    )(states, inputs[None], targets)
    square = shape(count, count)
    short = shape(count, count, dtype=BF16)
    thin_shape = shape(rows, count)
    solved = pl.pallas_call(
        functools.partial(inverse_kernel, reduced=reduced, half=half),
        out_shape=(short, short, square, short, short, thin_shape, thin_shape),
        in_specs=[vmem],
        out_specs=(vmem,) * 7,
        scratch_shapes=[hold(count, count), hold(count, count, dtype=BF16)],
        compiler_params=pltpu.CompilerParams(vmem_limit_bytes=LIMIT),
        name="local_inverse",
    )(packed)
    block = shape(rows, columns)
    after, duals, last, history = pl.pallas_call(
        functools.partial(second_kernel, reduced=reduced, half=half, width=width),
        out_shape=(block, block, block, shape(8, LANES)),
        in_specs=[vmem] * 8,
        out_specs=(vmem,) * 4,
        scratch_shapes=[
            hold(columns, count),
            hold(columns, count, dtype=BF16), hold(columns, count, dtype=BF16),
            hold(count, columns, dtype=BF16), hold(count, columns, dtype=BF16),
            hold(count, count), hold(count, count, dtype=BF16), hold(count, count, dtype=BF16),
            hold(count, count, dtype=BF16),
            hold(owners, half, wide), hold(owners, half, wide),
            hold(feats, slabs, half, wide), hold(feats, slabs, half, wide),
            hold(feats, half, wide), hold(feats, half + 1, wide),
            hold(owners, half, wide), hold(owners, half + 1, wide),
            dma((owners,)), dma((feats, slabs)), dma((feats, slabs)), dma((owners,)),
            dma((owners,)), dma((feats, slabs)), dma((feats, slabs)), dma((owners,)),
        ],
        compiler_params=pltpu.CompilerParams(vmem_limit_bytes=2 * LIMIT, collective_id=0, has_side_effects=True),
        name="second_and_averages",
    )(packed, *solved)
    shard = shape(half, width)
    spread_rows = shape(half, 1, width)
    after, duals, last, history = pl.pallas_call(
        last_kernel,
        out_shape=(spread_rows, spread_rows, shard, shape(2, 2)),
        in_specs=[vmem] * 4,
        out_specs=(vmem,) * 4,
        compiler_params=pltpu.CompilerParams(vmem_limit_bytes=4 * 2**20),
        name="outputs",
    )(after, duals, last, history)
    return (jnp.swapaxes(after, 0, 1), jnp.swapaxes(duals, 0, 1), last, history)


def solution(mesh):
    in_specs = (P(None, ("slab", "feat")), P(("slab", "feat")), P(None, ("slab", "feat")))
    out_specs = (P("slab", "feat", None), P("slab", "feat", None), P("feat", None), P())
    return jax.shard_map(shards, mesh=mesh, in_specs=in_specs, out_specs=out_specs, check_vma=False)
```

```python
import functools

import jax
import jax.numpy as jnp
from jax import lax
from jax.experimental import pallas as pl
from jax.experimental.pallas import tpu as pltpu
from jax.sharding import PartitionSpec as P

penalty = 1.0
LIMIT = 20 * 2**20
LANES = 128
NN = (((1,), (0,)), ((), ()))
NT = (((1,), (1,)), ((), ()))
TN = (((0,), (0,)), ((), ()))
F32 = jnp.float32
BF16 = jnp.bfloat16


def up(value, step):
    return -(-value // step) * step


def dot(left, right, dims=NN):
    return lax.dot_general(left.astype(BF16), right.astype(BF16), dims, preferred_element_type=F32)


def split(value):
    high = value.astype(BF16)
    return high, (value - high.astype(F32)).astype(BF16)


def thin(left, high, low, dims=NN):
    rows = left.shape[0]
    top = left.astype(BF16).astype(F32)
    both = jnp.concatenate([top, left - top], 0).astype(BF16)
    out = dot(both, high, dims) + dot(both, low, dims)
    return out[:rows] + out[rows:]


def eye_mask(size):
    return lax.broadcasted_iota(jnp.int32, (size, size), 0) == lax.broadcasted_iota(jnp.int32, (size, size), 1)


def eye(size):
    return jnp.where(eye_mask(size), 1.0, 0.0)


def invert_by_pivots(source, target):
    size = source.shape[0]
    target[...] = source[...]
    sub = lax.broadcasted_iota(jnp.int32, (size, 1), 0)
    lane = lax.broadcasted_iota(jnp.int32, (1, size), 1)

    def step(k, carry):
        row = target[pl.ds(k, 1), :]
        here = lane == k
        pivot = jnp.sum(jnp.where(here, row, 0.0), axis=1, keepdims=True)
        scaled = jnp.where(here, 1.0, row) / pivot
        whole = target[...]
        column = jnp.sum(jnp.where(here, whole, 0.0), axis=1, keepdims=True)
        column = jnp.where(sub == k, -1.0, column)
        kept = jnp.where(here | (sub == k), 0.0, whole)
        target[...] = kept - column * scaled
        return carry

    lax.fori_loop(0, size, step, 0)


def exchange_kernel(
    states, inputs, targets, all_s, all_u, all_t, near_s, near_u, near_t, local, send, recv
):
    feats = lax.axis_size("feat")
    core = lax.axis_index("feat")
    head = feats - 1
    own = states.shape[1]
    sources = (states, inputs, targets)
    nears = (near_s, near_u, near_t)
    alls = (all_s, all_u, all_t)

    def load(i, target):
        return pltpu.make_async_copy(sources[i], target, local.at[i])

    def move(i, f):
        return pltpu.make_async_remote_copy(
            src_ref=nears[i], dst_ref=alls[i].at[:, pl.ds(f * own, own)], send_sem=send.at[i], recv_sem=recv.at[f, i],
            device_id={"feat": head}, device_id_type=pl.DeviceIdType.MESH,
        )

    barrier = pltpu.get_barrier_semaphore()

    def greet(feat):
        pl.semaphore_signal(barrier, inc=1, device_id={"feat": feat}, device_id_type=pl.DeviceIdType.MESH)

    @pl.when(core == head)
    def _():
        for i in range(3):
            load(i, alls[i].at[:, pl.ds(head * own, own)]).start()
        for f in range(head):
            greet(f)
        pl.semaphore_wait(barrier, head)
        for i in range(3):
            load(i, alls[i].at[:, pl.ds(head * own, own)]).wait()
        for f in range(head):
            for i in range(3):
                move(i, f).wait_recv()

    for f in range(head):

        @pl.when(core == f)
        def _():
            for i in range(3):
                load(i, nears[i]).start()
            greet(head)
            pl.semaphore_wait(barrier, 1)
            for i in range(3):
                load(i, nears[i]).wait()
                move(i, f).start()
            for i in range(3):
                move(i, f).wait_send()


def stacked(value, orders):
    parts = []
    rest = value
    for _ in range(1 + max(max(order) for order in orders)):
        high = rest.astype(BF16).astype(F32)
        parts.append(high)
        rest = rest - high
    left = jnp.concatenate([parts[i] for i, _ in orders], 0)
    right = jnp.concatenate([parts[j] for _, j in orders], 0)
    return left.astype(BF16), right.astype(BF16)


def inverse_kernel(all_s, all_u, high_a, low_a, inverse, high_x, low_x, system, shifted):
    reduced, count = all_s.shape
    edge = LANES
    spans = [slice(k, k + edge) for k in range(0, count, edge)]

    def solve():
        s = all_s[...]
        sub = lax.broadcasted_iota(jnp.int32, (8, count), 0)
        last = jnp.where(sub == 0, all_u[...], jnp.where(sub == 1, 1.0, 0.0)) * (1.0 / count) ** 0.5
        left, right = stacked(s * (0.5 / count) ** 0.25, ((0, 0), (0, 1), (1, 0), (0, 2), (2, 0), (1, 1)))
        extra = jnp.concatenate([s * s * (0.5 / count) ** 0.5, last], 0)
        left2, right2 = stacked(extra, ((0, 0), (0, 1), (1, 0)))
        sums = [jnp.zeros((8, edge), F32)] * len(spans)
        for p, down in enumerate(spans):
            inner = dot(left[:, down], right, TN)
            other = dot(left2[:, down], right2, TN)
            for q, across in enumerate(spans):
                part = inner[:, across]
                part = part * (part + (2.0 / count) ** 0.5) + other[:, across]
                if p == q:
                    part = part + jnp.where(eye_mask(edge), penalty, 0.0)
                system[down, across] = part
                high_a[down, across], low_a[down, across] = split(part)
                sums[q] = sums[q] + jnp.abs(part).reshape(edge // 8, 8, edge).sum(0)
        sums = functools.reduce(jnp.maximum, [jnp.sum(part, axis=0, keepdims=True) for part in sums])
        high = jnp.max(sums) / penalty
        delta = (high - 1.0) / (high + 1.0)
        alpha = 2.0 / ((1.0 + high) * penalty)
        c = 2.0 / (2.0 - delta * delta)
        for p, down in enumerate(spans):
            for q, across in enumerate(spans):
                part = (-c * alpha * alpha) * system[down, across]
                if p == q:
                    part = part + jnp.where(eye_mask(edge), 2.0 * c * alpha, 0.0)
                inverse[down, across] = part
        delta = delta * delta / (2.0 - delta * delta)

        def coarse(state):
            step, delta = state
            x = inverse[...].astype(BF16)
            shifted[...] = dot(high_a[...], x).astype(BF16)
            c = 2.0 / (2.0 - delta * delta)
            inverse[...] = c * (2.0 * inverse[...] - dot(x, shifted[...]))
            return step + 1, delta * delta / (2.0 - delta * delta)

        lax.while_loop(lambda state: (state[1] > 0.085) & (state[0] < 12), coarse, (0, delta))

        mixed = (lax.broadcasted_iota(jnp.int32, (8, count), 1) + 1) * (sub * 40503 + 30011)
        mixed = (mixed ^ (mixed >> 7)) * 9973
        signs = jnp.where(((mixed >> 9) & 1) == 1, 1.0, -1.0)

        x = inverse[...].astype(BF16)
        ah, al = high_a[...], low_a[...]
        shifted[...] = (eye(count) - (dot(ah, x) + dot(al, x))).astype(BF16)
        once = signs - thin(dot(signs, x), ah, al)
        high_once, low_once = split(once)
        twice = once - thin(dot(high_once, x) + dot(low_once, x), ah, al)
        inverse[...] = x.astype(F32) + dot(x, shifted[...])
        high_x[...], low_x[...] = split(inverse[...])
        worst = jnp.sum(twice * twice) * (1.0 / 8.0)

        def polish(state):
            step, _ = state
            ah, al, xh, xl = high_a[...], low_a[...], high_x[...], low_x[...]
            shifted[...] = (eye(count) - (dot(ah, xh) + (dot(ah, xl) + dot(al, xh)))).astype(BF16)
            once = signs - thin(thin(signs, xh, xl), ah, al)
            twice = once - thin(thin(once, xh, xl), ah, al)
            inverse[...] = inverse[...] + dot(xh, shifted[...])
            high_x[...], low_x[...] = split(inverse[...])
            return step + 1, jnp.sum(twice * twice) * (1.0 / 8.0)

        _, worst = lax.while_loop(
            lambda state: jnp.logical_not(state[1] < 0.012) & (state[0] < 6), polish, (0, worst)
        )

        @pl.when(jnp.logical_not(worst < 0.012))
        def _():
            invert_by_pivots(system, inverse)
            high_x[...], low_x[...] = split(inverse[...])

    pl.when(lax.axis_index("feat") == lax.axis_size("feat") - 1)(solve)


def build_features(all_s, all_u, phi):
    reduced, count = all_s.shape
    row = reduced
    phi[0:reduced, :] = all_s[...]
    for i in range(reduced):
        phi[row : row + reduced - i, :] = all_s[i : i + 1, :] * all_s[i:reduced, :]
        row += reduced - i
    phi[row : row + 1, :] = all_u[...]
    phi[row + 1 : row + 2, :] = jnp.ones((1, count), F32)
    if row + 2 < phi.shape[0]:
        phi[row + 2 :, :] = jnp.zeros((phi.shape[0] - row - 2, count), F32)


def lanes_of(value):
    return jnp.sum(value.reshape(-1, value.shape[-1]), axis=0, keepdims=True)


def second_kernel(
    all_s, all_u, all_t, high_a, low_a, inverse, high_x, low_x, after, duals, last, history,
    phi, high_p, low_p, high_w, low_w, better, high_b, low_b, gap, answer,
    own1, own2, land1, land2, out1, out2, mean1, mean2, mine, ship, span,
    send1, recv1, spread1, got1, send2, recv2, spread2, got2, ship_send, ship_recv,
    *, width,
):
    slabs = lax.axis_size("slab")
    feats = lax.axis_size("feat")
    me = lax.axis_index("slab")
    core = lax.axis_index("feat")
    owners, reduced, wide = own1.shape
    half = reduced // feats
    count = all_s.shape[1]
    base = (slabs - owners) // 2
    head = feats - 1
    spot = jnp.clip(me - base, 0, owners - 1)
    leading = core == head
    inside = (me >= base) & (me < base + owners)

    def copy(source, target, send, recv, slab, feat):
        return pltpu.make_async_remote_copy(
            src_ref=source, dst_ref=target, send_sem=send, recv_sem=recv,
            device_id={"slab": slab, "feat": feat}, device_id_type=pl.DeviceIdType.MESH,
        )

    def arrived(target, size, sem):
        part = target.at[pl.ds(0, size)]
        copy(part, part, sem, sem, me, core).wait_recv()

    def departed(source, size, sem):
        part = source.at[pl.ds(0, size)]
        copy(part, part, sem, sem, me, core).wait_send()

    def each(order, body):
        if len(order) <= 16:
            for d in order:
                body(d)
            return

        def step(d, carry):
            body(d)
            return carry

        lax.fori_loop(min(order), max(order) + 1, step, 0)

    far = sorted(range(1, slabs), key=lambda d: -min(d, slabs - d))

    def slab_of(d):
        return lax.rem(me + d, slabs)

    def split_on(flag, yes, no):
        pl.when(flag)(yes)
        pl.when(jnp.logical_not(flag))(no)

    barrier = pltpu.get_barrier_semaphore()

    def greet(slab, feat):
        pl.semaphore_signal(
            barrier, inc=1, device_id={"slab": slab, "feat": feat}, device_id_type=pl.DeviceIdType.MESH
        )

    @pl.when(leading & inside)
    def _():
        for f in range(feats):
            each(far, lambda d, f=f: greet(slab_of(d), f))
        for f in range(head):
            greet(me, f)

    @pl.when(jnp.logical_not(leading & inside))
    def _():
        def one(k):
            greet(base + k, head)

        each(range(owners), one)

    @pl.when(leading & jnp.logical_not(inside))
    def _():
        for f in range(head):
            greet(me, f)

    @pl.when(jnp.logical_not(leading) & jnp.logical_not(inside))
    def _():
        greet(me, head)

    def scatter(source, landing, send, recv):
        def start(k):
            @pl.when(me != base + k)
            def _():
                copy(source.at[k], landing.at[me], send, recv, base + k, head).start()

        each(range(owners), start)

    def joined(buffer, rows):
        return jnp.concatenate([buffer[k][:rows] for k in range(owners)], 1)

    def owner_first():
        land1[me] = own1[spot]
        arrived(land1, slabs - 1, recv1)
        out1[...] = land1[...].sum(0) * (1.0 / slabs)
        each(far, lambda d: copy(out1, mean1.at[spot], spread1, got1, slab_of(d), head).start())
        mean1[spot] = out1[...]

    def owner_second():
        old = out1[...]
        primal1 = lanes_of(jnp.square(land1[...] - old[None]))
        dual1 = lanes_of(jnp.square(old))
        land2[me] = own2[spot]
        arrived(land2, slabs - 1, recv2)
        new = land2[...].sum(0) * (1.0 / slabs)
        primal2 = lanes_of(jnp.square(land2[...] - new[None]))
        dual2 = lanes_of(jnp.square(new - old))
        scale = slabs * penalty * penalty
        stats = jnp.concatenate([primal1, primal2, dual1 * scale, dual2 * scale], 0)
        for f in range(feats):
            out2[f, 0:half] = new[f * half : (f + 1) * half]
            out2[f, half : half + 4] = stats
        for d in far:
            for f in range(feats):
                copy(out2.at[f], mean2.at[spot], spread2, got2, slab_of(d), f).start()
        for f in range(head):
            copy(out2.at[f], mean2.at[spot], spread2, got2, me, f).start()
        mean2[spot] = out2[head]

    def leader():
        ah, al, xh, xl = high_a[...], low_a[...], high_x[...], low_x[...]
        b = all_t[...] * (1.0 / count)
        build_features(all_s, all_u, phi)
        high_p[...], low_p[...] = split(phi[...])
        y = thin(b, xh, xl)
        y = y + thin(b - thin(y, ah, al), xh, xl)
        y = y + thin(b - thin(y, ah, al), xh, xl)
        answer[...] = y
        start_value = thin(y, high_p[...], low_p[...], NT)
        for k in range(owners):
            own1[k] = start_value[:, k * wide : (k + 1) * wide]
        split_on(
            inside,
            lambda: pl.semaphore_wait(barrier, slabs * feats - 1),
            lambda: pl.semaphore_wait(barrier, owners + feats - 1),
        )
        scatter(own1, land1, send1, recv1)

        gap[...] = (eye(count) - (dot(ah, xh) + (dot(ah, xl) + dot(al, xh)))).astype(BF16)
        better[...] = inverse[...] + dot(xh, gap[...])
        high_b[...], low_b[...] = split(better[...])
        bh, bl = high_b[...], low_b[...]
        gap[...] = (eye(count) - (dot(ah, bh) + (dot(ah, bl) + dot(al, bh)))).astype(BF16)
        better[...] = better[...] + dot(bh, gap[...])
        high_b[...], low_b[...] = split(better[...])
        pl.when(inside)(owner_first)
        weights = dot(high_b[...], high_p[...], NT) + (
            dot(high_b[...], low_p[...], NT) + dot(low_b[...], high_p[...], NT)
        )
        high_w[...], low_w[...] = split(weights)

        split_on(
            inside,
            lambda: arrived(mean1, owners - 1, got1),
            lambda: arrived(mean1, owners, got1),
        )
        first = joined(own1, reduced)
        mean = joined(mean1, reduced)
        v = thin(mean, high_p[...], low_p[...]) * (2.0 / (count * penalty)) + answer[...]
        result = first + 2.0 * mean - thin(v, high_w[...], low_w[...])
        for k in range(owners):
            own2[k] = result[:, k * wide : (k + 1) * wide]
        scatter(own2, land2, send2, recv2)
        change = (first - mean) + result
        for f in range(head):
            ship[f, 0] = result[f * half : (f + 1) * half]
            ship[f, 1] = change[f * half : (f + 1) * half]
            copy(ship.at[f], mine, ship_send.at[f], ship_recv, me, f).start()
        mine[0] = result[head * half :]
        mine[1] = change[head * half :]
        pl.when(inside)(owner_second)

        def sent(size):
            departed(own1, size, send1)
            departed(own2, size, send2)

        split_on(inside, lambda: sent(owners - 1), lambda: sent(owners))
        for f in range(head):
            copy(ship.at[f], mine, ship_send.at[f], ship_recv, me, core).wait_send()

    def follower():
        split_on(
            inside,
            lambda: pl.semaphore_wait(barrier, owners),
            lambda: pl.semaphore_wait(barrier, owners + 1),
        )
        copy(ship.at[0], mine, ship_send.at[0], ship_recv, me, core).wait_recv()

    split_on(leading, leader, follower)
    split_on(
        leading & inside,
        lambda: arrived(mean2, owners - 1, got2),
        lambda: arrived(mean2, owners, got2),
    )
    new = joined(mean2, half)
    after[...] = mine[0]
    last[...] = new
    duals[...] = mine[1] - new
    sums = mean2[0][half : half + 4]
    for k in range(1, owners):
        sums = sums + mean2[k][half : half + 4]
    sums = jnp.sum(sums, axis=1, keepdims=True)
    history[...] = jnp.broadcast_to(jnp.sqrt(sums * (1.0 / (slabs * reduced * width))), history.shape)

    @pl.when(leading & inside)
    def _():
        departed(land1, slabs - 1, spread1)
        departed(span, slabs * feats - 1, spread2)


def last_kernel(after, duals, last, history, out_after, out_duals, out_last, out_history):
    half, width = out_last.shape
    for r in range(half):
        out_after[r] = after[r : r + 1, :width]
        out_duals[r] = duals[r : r + 1, :width]
    out_last[...] = last[:, :width]
    for r in range(2):
        out_history[r : r + 1, :] = jnp.concatenate([history[2 * r + k : 2 * r + k + 1, 0:1] for k in range(2)], 1)


def shards(states, inputs, targets):
    reduced, own = states.shape
    feats = lax.axis_size("feat")
    slabs = lax.axis_size("slab")
    half = reduced // feats
    width = reduced + reduced * (reduced + 1) // 2 + 2
    count = own * feats
    tiles = up(width, LANES) // LANES
    wide = -(-tiles // slabs) * LANES
    columns = up(width, wide)
    owners = columns // wide
    vmem = pl.BlockSpec(memory_space=pltpu.VMEM)
    dma = pltpu.SemaphoreType.DMA

    def shape(*sizes, dtype=F32):
        return jax.ShapeDtypeStruct(sizes, dtype)

    def hold(*sizes, dtype=F32):
        return pltpu.VMEM(sizes, dtype)

    gathered = pl.pallas_call(
        exchange_kernel,
        out_shape=(shape(reduced, count), shape(1, count), shape(reduced, count)),
        in_specs=[pl.BlockSpec(memory_space=pltpu.HBM)] * 3,
        out_specs=(vmem,) * 3,
        scratch_shapes=[
            hold(reduced, own), hold(1, own), hold(reduced, own), dma((3,)), dma((3,)), dma((feats, 3)),
        ],
        compiler_params=pltpu.CompilerParams(vmem_limit_bytes=LIMIT, collective_id=1, has_side_effects=True),
        name="exchange",
    )(states, inputs[None], targets)
    square = shape(count, count)
    short = shape(count, count, dtype=BF16)
    solved = pl.pallas_call(
        inverse_kernel,
        out_shape=(short, short, square, short, short),
        in_specs=[vmem] * 2,
        out_specs=(vmem,) * 5,
        scratch_shapes=[hold(count, count), hold(count, count, dtype=BF16)],
        compiler_params=pltpu.CompilerParams(vmem_limit_bytes=LIMIT),
        name="local_inverse",
    )(gathered[0], gathered[1])
    block = shape(half, columns)
    after, duals, last, history = pl.pallas_call(
        functools.partial(second_kernel, width=width),
        out_shape=(block, block, block, shape(4, LANES)),
        in_specs=[vmem] * 8,
        out_specs=(vmem,) * 4,
        scratch_shapes=[
            hold(columns, count),
            hold(columns, count, dtype=BF16), hold(columns, count, dtype=BF16),
            hold(count, columns, dtype=BF16), hold(count, columns, dtype=BF16),
            hold(count, count), hold(count, count, dtype=BF16), hold(count, count, dtype=BF16),
            hold(count, count, dtype=BF16), hold(reduced, count),
            hold(owners, reduced, wide), hold(owners, reduced, wide),
            hold(slabs, reduced, wide), hold(slabs, reduced, wide),
            hold(reduced, wide), hold(feats, half + 4, wide),
            hold(owners, reduced, wide), hold(owners, half + 4, wide),
            hold(2, half, columns), hold(max(feats - 1, 1), 2, half, columns),
            hold(slabs * feats, half + 4, wide),
            dma, dma, dma, dma, dma, dma, dma, dma, dma((max(feats - 1, 1),)), dma,
        ],
        compiler_params=pltpu.CompilerParams(vmem_limit_bytes=2 * LIMIT, collective_id=0, has_side_effects=True),
        name="second_and_averages",
    )(*gathered, *solved)
    shard = shape(half, width)
    spread_rows = shape(half, 1, width)
    after, duals, last, history = pl.pallas_call(
        last_kernel,
        out_shape=(spread_rows, spread_rows, shard, shape(2, 2)),
        in_specs=[vmem] * 4,
        out_specs=(vmem,) * 4,
        compiler_params=pltpu.CompilerParams(vmem_limit_bytes=4 * 2**20),
        name="outputs",
    )(after, duals, last, history)
    return (jnp.swapaxes(after, 0, 1), jnp.swapaxes(duals, 0, 1), last, history)


def solution(mesh):
    in_specs = (P(None, ("slab", "feat")), P(("slab", "feat")), P(None, ("slab", "feat")))
    out_specs = (P("slab", "feat", None), P("slab", "feat", None), P("feat", None), P())
    return jax.shard_map(shards, mesh=mesh, in_specs=in_specs, out_specs=out_specs, check_vma=False)
```

```python
import functools

import jax
import jax.numpy as jnp
from jax import lax
from jax.experimental import pallas as pl
from jax.experimental.pallas import tpu as pltpu
from jax.sharding import PartitionSpec as P

penalty = 1.0
LIMIT = 20 * 2**20
LANES = 128
STEPS = 4
EASY = 400.0
NN = (((1,), (0,)), ((), ()))
NT = (((1,), (1,)), ((), ()))
TN = (((0,), (0,)), ((), ()))
F32 = jnp.float32
BF16 = jnp.bfloat16


def up(value, step):
    return -(-value // step) * step


def dot(left, right, dims=NN):
    return lax.dot_general(left.astype(BF16), right.astype(BF16), dims, preferred_element_type=F32)


def split(value):
    high = value.astype(BF16)
    return high, (value - high.astype(F32)).astype(BF16)


def thin(left, high, low, dims=NN):
    rows = left.shape[0]
    top = left.astype(BF16).astype(F32)
    both = jnp.concatenate([top, left - top], 0).astype(BF16)
    out = dot(both, high, dims) + dot(both, low, dims)
    return out[:rows] + out[rows:]


def eye_mask(size):
    return lax.broadcasted_iota(jnp.int32, (size, size), 0) == lax.broadcasted_iota(jnp.int32, (size, size), 1)


def eye(size):
    return jnp.where(eye_mask(size), 1.0, 0.0)


def invert_by_pivots(source, target):
    size = source.shape[0]
    target[...] = source[...]
    sub = lax.broadcasted_iota(jnp.int32, (size, 1), 0)
    lane = lax.broadcasted_iota(jnp.int32, (1, size), 1)

    def step(k, carry):
        row = target[pl.ds(k, 1), :]
        here = lane == k
        pivot = jnp.sum(jnp.where(here, row, 0.0), axis=1, keepdims=True)
        scaled = jnp.where(here, 1.0, row) / pivot
        whole = target[...]
        column = jnp.sum(jnp.where(here, whole, 0.0), axis=1, keepdims=True)
        column = jnp.where(sub == k, -1.0, column)
        kept = jnp.where(here | (sub == k), 0.0, whole)
        target[...] = kept - column * scaled
        return carry

    lax.fori_loop(0, size, step, 0)


def exchange_kernel(
    states, inputs, targets, all_s, all_u, all_t, near_s, near_u, near_t, local, send, recv
):
    feats = lax.axis_size("feat")
    core = lax.axis_index("feat")
    head = feats - 1
    own = states.shape[1]
    sources = (states, inputs, targets)
    nears = (near_s, near_u, near_t)
    alls = (all_s, all_u, all_t)

    def load(i, target):
        return pltpu.make_async_copy(sources[i], target, local.at[i])

    def move(i, f):
        return pltpu.make_async_remote_copy(
            src_ref=nears[i], dst_ref=alls[i].at[:, pl.ds(f * own, own)], send_sem=send.at[i], recv_sem=recv.at[f, i],
            device_id={"feat": head}, device_id_type=pl.DeviceIdType.MESH,
        )

    barrier = pltpu.get_barrier_semaphore()

    def greet(feat):
        pl.semaphore_signal(barrier, inc=1, device_id={"feat": feat}, device_id_type=pl.DeviceIdType.MESH)

    @pl.when(core == head)
    def _():
        for i in range(3):
            load(i, alls[i].at[:, pl.ds(head * own, own)]).start()
        for f in range(head):
            greet(f)
        pl.semaphore_wait(barrier, head)
        for i in range(3):
            load(i, alls[i].at[:, pl.ds(head * own, own)]).wait()
        for f in range(head):
            for i in range(3):
                move(i, f).wait_recv()

    for f in range(head):

        @pl.when(core == f)
        def _():
            for i in range(3):
                load(i, nears[i]).start()
            greet(head)
            pl.semaphore_wait(barrier, 1)
            for i in range(3):
                load(i, nears[i]).wait()
                move(i, f).start()
            for i in range(3):
                move(i, f).wait_send()


def stacked(value, orders):
    parts = []
    rest = value
    for _ in range(1 + max(max(order) for order in orders)):
        high = rest.astype(BF16).astype(F32)
        parts.append(high)
        rest = rest - high
    left = jnp.concatenate([parts[i] for i, _ in orders], 0)
    right = jnp.concatenate([parts[j] for _, j in orders], 0)
    return left.astype(BF16), right.astype(BF16)


def newton_scale(delta):
    return 2.0 / (2.0 - delta * delta), delta * delta / (2.0 - delta * delta)


def inverse_kernel(all_s, all_u, high_a, low_a, inverse, info, system, shifted, high_x, low_x):
    reduced, count = all_s.shape
    edge = LANES
    spans = [slice(k, k + edge) for k in range(0, count, edge)]

    def solve():
        s = all_s[...]
        sub = lax.broadcasted_iota(jnp.int32, (8, count), 0)
        last = jnp.where(sub == 0, all_u[...], jnp.where(sub == 1, 1.0, 0.0)) * (1.0 / count) ** 0.5
        left, right = stacked(s * (0.5 / count) ** 0.25, ((0, 0), (0, 1), (1, 0), (0, 2), (2, 0), (1, 1)))
        extra = jnp.concatenate([s * s * (0.5 / count) ** 0.5, last], 0)
        left2, right2 = stacked(extra, ((0, 0), (0, 1), (1, 0)))
        sums = [jnp.zeros((8, edge), F32)] * len(spans)
        for p, down in enumerate(spans):
            inner = dot(left[:, down], right, TN)
            other = dot(left2[:, down], right2, TN)
            for q, across in enumerate(spans):
                part = inner[:, across]
                part = part * (part + (2.0 / count) ** 0.5) + other[:, across]
                if p == q:
                    part = part + jnp.where(eye_mask(edge), penalty, 0.0)
                system[down, across] = part
                high_a[down, across], low_a[down, across] = split(part)
                sums[q] = sums[q] + jnp.abs(part).reshape(edge // 8, 8, edge).sum(0)
        sums = functools.reduce(jnp.maximum, [jnp.sum(part, axis=0, keepdims=True) for part in sums])
        high = jnp.max(sums) / penalty
        delta = (high - 1.0) / (high + 1.0)
        alpha = 2.0 / ((1.0 + high) * penalty)
        c, later = newton_scale(delta)
        for p, down in enumerate(spans):
            for q, across in enumerate(spans):
                part = (-c * alpha * alpha) * system[down, across]
                if p == q:
                    part = part + jnp.where(eye_mask(edge), 2.0 * c * alpha, 0.0)
                inverse[down, across] = part
        hard = jnp.logical_not(high <= EASY)
        lane = lax.broadcasted_iota(jnp.int32, (1, LANES), 1)
        info[...] = jnp.where(lane == 0, later, jnp.where(hard, 1.0, 0.0))

        @pl.when(hard)
        def _():
            careful(later)

    def careful(delta):
        sub = lax.broadcasted_iota(jnp.int32, (8, count), 0)
        mixed = (lax.broadcasted_iota(jnp.int32, (8, count), 1) + 1) * (sub * 40503 + 30011)
        mixed = (mixed ^ (mixed >> 7)) * 9973
        signs = jnp.where(((mixed >> 9) & 1) == 1, 1.0, -1.0)

        def coarse(state):
            step, delta = state
            x = inverse[...].astype(BF16)
            shifted[...] = dot(high_a[...], x).astype(BF16)
            c, later = newton_scale(delta)
            inverse[...] = c * (2.0 * inverse[...] - dot(x, shifted[...]))
            return step + 1, later

        lax.while_loop(lambda state: (state[1] > 0.085) & (state[0] < 12), coarse, (0, delta))

        def polish(state):
            step, _ = state
            high_x[...], low_x[...] = split(inverse[...])
            ah, al, xh, xl = high_a[...], low_a[...], high_x[...], low_x[...]
            shifted[...] = (eye(count) - (dot(ah, xh) + (dot(ah, xl) + dot(al, xh)))).astype(BF16)
            once = signs - thin(thin(signs, xh, xl), ah, al)
            twice = once - thin(thin(once, xh, xl), ah, al)
            inverse[...] = inverse[...] + dot(xh, shifted[...])
            return step + 1, jnp.sum(twice * twice) * (1.0 / 8.0)

        _, worst = lax.while_loop(
            lambda state: jnp.logical_not(state[1] < 0.001) & (state[0] < 8), polish, (0, jnp.float32(1e9))
        )

        @pl.when(jnp.logical_not(worst < 0.001))
        def _():
            invert_by_pivots(system, inverse)

    pl.when(lax.axis_index("feat") == lax.axis_size("feat") - 1)(solve)


def build_features(all_s, all_u, phi):
    reduced, count = all_s.shape
    row = reduced
    phi[0:reduced, :] = all_s[...]
    for i in range(reduced):
        phi[row : row + reduced - i, :] = all_s[i : i + 1, :] * all_s[i:reduced, :]
        row += reduced - i
    phi[row : row + 1, :] = all_u[...]
    phi[row + 1 : row + 2, :] = jnp.ones((1, count), F32)
    if row + 2 < phi.shape[0]:
        phi[row + 2 :, :] = jnp.zeros((phi.shape[0] - row - 2, count), F32)


def lanes_of(value):
    return jnp.sum(value.reshape(-1, value.shape[-1]), axis=0, keepdims=True)


def second_kernel(
    all_s, all_u, all_t, high_a, low_a, inverse, info, after, duals, last, history,
    phi, high_p, low_p, high_w, low_w, better, high_b, low_b, gap, answer,
    own1, own2, land1, land2, out1, out2, mean1, mean2, mine, ship, span,
    send1, recv1, spread1, got1, send2, recv2, spread2, got2, ship_send, ship_recv,
    *, width, first_owners, second_owners, order,
):
    slabs = lax.axis_size("slab")
    feats = lax.axis_size("feat")
    me = lax.axis_index("slab")
    core = lax.axis_index("feat")
    owners, reduced, wide = own1.shape
    half = reduced // feats
    count = all_s.shape[1]
    head = feats - 1
    leading = core == head
    everyones = sorted(set(first_owners) | set(second_owners))

    def among(slab_list):
        return functools.reduce(jnp.logical_or, [me == slab for slab in slab_list])

    def place_in(slab_list):
        return functools.reduce(lambda a, b: a + b, [jnp.where(me == slab, k, 0) for k, slab in enumerate(slab_list)])

    inside, inside1, inside2 = among(everyones), among(first_owners), among(second_owners)
    spot1, spot2 = place_in(first_owners), place_in(second_owners)

    def copy(source, target, send, recv, slab, feat):
        return pltpu.make_async_remote_copy(
            src_ref=source, dst_ref=target, send_sem=send, recv_sem=recv,
            device_id={"slab": slab, "feat": feat}, device_id_type=pl.DeviceIdType.MESH,
        )

    def arrived(target, size, sem):
        part = target.at[pl.ds(0, size)]
        copy(part, part, sem, sem, me, core).wait_recv()

    def departed(source, size, sem):
        part = source.at[pl.ds(0, size)]
        copy(part, part, sem, sem, me, core).wait_send()

    def each(order, body):
        if len(order) <= 16:
            for d in order:
                body(d)
            return

        def step(d, carry):
            body(d)
            return carry

        lax.fori_loop(min(order), max(order) + 1, step, 0)

    far = sorted(range(1, slabs), key=lambda d: -min(d, slabs - d))

    def slab_of(d):
        return lax.rem(me + d, slabs)

    def split_on(flag, yes, no):
        pl.when(flag)(yes)
        pl.when(jnp.logical_not(flag))(no)

    barrier = pltpu.get_barrier_semaphore()

    def greet(slab, feat):
        pl.semaphore_signal(
            barrier, inc=1, device_id={"slab": slab, "feat": feat}, device_id_type=pl.DeviceIdType.MESH
        )

    @pl.when(leading & inside)
    def _():
        for f in range(feats):
            each(far, lambda d, f=f: greet(slab_of(d), f))
        for f in range(head):
            greet(me, f)

    @pl.when(jnp.logical_not(leading & inside))
    def _():
        for slab in everyones:
            greet(slab, head)

    @pl.when(leading & jnp.logical_not(inside))
    def _():
        for f in range(head):
            greet(me, f)

    @pl.when(jnp.logical_not(leading) & jnp.logical_not(inside))
    def _():
        greet(me, head)

    def scatter(source, landing, send, recv, slab_list):
        for k, slab in enumerate(slab_list):

            @pl.when(me != slab)
            def _():
                copy(source.at[k], landing.at[me], send, recv, slab, head).start()

    def joined(buffer, rows):
        return jnp.concatenate([buffer[k][:rows] for k in range(owners)], 1)

    def owner_first():
        land1[me] = own1[spot1]
        arrived(land1, slabs - 1, recv1)
        out1[...] = land1[...].sum(0) * (1.0 / slabs)
        each(far, lambda d: copy(out1, mean1.at[spot1], spread1, got1, slab_of(d), head).start())
        mean1[spot1] = out1[...]

    def owner_second():
        old = mean1[spot2]
        dual1 = lanes_of(jnp.square(old))
        land2[me] = own2[spot2]
        arrived(land2, slabs - 1, recv2)
        whole = land2[...].sum(0)
        new = whole[:reduced] * (1.0 / slabs)
        primal2 = lanes_of(jnp.square(land2[:, 0:reduced] - new[None]))
        dual2 = lanes_of(jnp.square(new - old))
        scale = slabs * penalty * penalty
        stats = jnp.concatenate([whole[reduced : reduced + 1], primal2, dual1 * scale, dual2 * scale], 0)
        for f in range(feats):
            out2[f, 0:half] = new[f * half : (f + 1) * half]
            out2[f, half : half + 4] = stats

        def one(slab):
            for f in range(feats):

                @pl.when((me != slab) | (f != head))
                def _():
                    copy(out2.at[f], mean2.at[spot2], spread2, got2, slab, f).start()

        for slab in order:
            one(slab)
        mean2[spot2] = out2[head]

    def leader():
        ah, al = high_a[...], low_a[...]
        delta = info[0:1, 0:1]
        kept = info[0:1, 1:2] > 0.5
        better[...] = inverse[...]

        def coarse(step, delta):
            x = better[...].astype(BF16)
            gap[...] = dot(high_a[...], x).astype(BF16)
            c, later = newton_scale(delta)
            value = better[...]
            better[...] = jnp.where(kept, value, c * (2.0 * value - dot(x, gap[...])))
            return later

        lax.fori_loop(0, STEPS, coarse, delta)
        b = all_t[...] * (1.0 / count)
        build_features(all_s, all_u, phi)
        high_p[...], low_p[...] = split(phi[...])
        x = better[...].astype(BF16)
        gap[...] = (eye(count) - (dot(ah, x) + dot(al, x))).astype(BF16)
        better[...] = jnp.where(kept, better[...], x.astype(F32) + dot(x, gap[...]))
        high_b[...], low_b[...] = split(better[...])
        xh, xl = high_b[...], low_b[...]
        y = thin(b, xh, xl)
        y = y + thin(b - thin(y, ah, al), xh, xl)
        y = y + thin(b - thin(y, ah, al), xh, xl)
        answer[...] = y
        start_value = thin(y, high_p[...], low_p[...], NT)
        for k in range(owners):
            own1[k] = start_value[:, k * wide : (k + 1) * wide]
        split_on(
            inside,
            lambda: pl.semaphore_wait(barrier, slabs * feats - 1),
            lambda: pl.semaphore_wait(barrier, len(everyones) + feats - 1),
        )
        scatter(own1, land1, send1, recv1, first_owners)

        gap[...] = (eye(count) - (dot(ah, xh) + (dot(ah, xl) + dot(al, xh)))).astype(BF16)
        better[...] = better[...] + dot(xh, gap[...])
        high_b[...], low_b[...] = split(better[...])
        bh, bl = high_b[...], low_b[...]
        gap[...] = (eye(count) - (dot(ah, bh) + (dot(ah, bl) + dot(al, bh)))).astype(BF16)
        better[...] = better[...] + dot(bh, gap[...])
        high_b[...], low_b[...] = split(better[...])
        pl.when(inside1)(owner_first)
        weights = dot(high_b[...], high_p[...], NT) + (
            dot(high_b[...], low_p[...], NT) + dot(low_b[...], high_p[...], NT)
        )
        high_w[...], low_w[...] = split(weights)

        split_on(
            inside1,
            lambda: arrived(mean1, owners - 1, got1),
            lambda: arrived(mean1, owners, got1),
        )
        first = joined(own1, reduced)
        mean = joined(mean1, reduced)
        v = thin(mean, high_p[...], low_p[...]) * (2.0 / (count * penalty)) + answer[...]
        result = first + 2.0 * mean - thin(v, high_w[...], low_w[...])
        primal1 = jnp.sum(jnp.square(first - mean), axis=0, keepdims=True)
        for k in range(owners):
            own2[k, 0:reduced] = result[:, k * wide : (k + 1) * wide]
            own2[k, reduced : reduced + 1] = primal1[:, k * wide : (k + 1) * wide]
        scatter(own2, land2, send2, recv2, second_owners)
        change = (first - mean) + result
        for f in range(head):
            ship[f, 0] = result[f * half : (f + 1) * half]
            ship[f, 1] = change[f * half : (f + 1) * half]
            copy(ship.at[f], mine, ship_send.at[f], ship_recv, me, f).start()
        mine[0] = result[head * half :]
        mine[1] = change[head * half :]
        pl.when(inside2)(owner_second)

        split_on(inside1, lambda: departed(own1, owners - 1, send1), lambda: departed(own1, owners, send1))
        split_on(inside2, lambda: departed(own2, owners - 1, send2), lambda: departed(own2, owners, send2))
        for f in range(head):
            copy(ship.at[f], mine, ship_send.at[f], ship_recv, me, core).wait_send()

    def follower():
        split_on(
            inside,
            lambda: pl.semaphore_wait(barrier, len(everyones)),
            lambda: pl.semaphore_wait(barrier, len(everyones) + 1),
        )
        copy(ship.at[0], mine, ship_send.at[0], ship_recv, me, core).wait_recv()

    split_on(leading, leader, follower)
    split_on(
        leading & inside2,
        lambda: arrived(mean2, owners - 1, got2),
        lambda: arrived(mean2, owners, got2),
    )
    new = joined(mean2, half)
    after[...] = mine[0]
    last[...] = new
    duals[...] = mine[1] - new
    sums = mean2[0][half : half + 4]
    for k in range(1, owners):
        sums = sums + mean2[k][half : half + 4]
    sums = jnp.sum(sums, axis=1, keepdims=True)
    history[...] = jnp.broadcast_to(jnp.sqrt(sums * (1.0 / (slabs * reduced * width))), history.shape)

    @pl.when(leading & inside1)
    def _():
        departed(land1, slabs - 1, spread1)

    @pl.when(leading & inside2)
    def _():
        departed(span, slabs * feats - 1, spread2)


def last_kernel(after, duals, last, history, out_after, out_duals, out_last, out_history):
    half, width = out_last.shape
    for r in range(half):
        out_after[r] = after[r : r + 1, :width]
        out_duals[r] = duals[r : r + 1, :width]
    out_last[...] = last[:, :width]
    for r in range(2):
        out_history[r : r + 1, :] = jnp.concatenate([history[2 * r + k : 2 * r + k + 1, 0:1] for k in range(2)], 1)


def shards(states, inputs, targets, *, spots):
    reduced, own = states.shape
    feats = lax.axis_size("feat")
    slabs = lax.axis_size("slab")
    half = reduced // feats
    width = reduced + reduced * (reduced + 1) // 2 + 2
    count = own * feats
    tiles = up(width, LANES) // LANES
    wide = -(-tiles // slabs) * LANES
    columns = up(width, wide)
    owners = columns // wide
    vmem = pl.BlockSpec(memory_space=pltpu.VMEM)
    dma = pltpu.SemaphoreType.DMA

    def shape(*sizes, dtype=F32):
        return jax.ShapeDtypeStruct(sizes, dtype)

    def hold(*sizes, dtype=F32):
        return pltpu.VMEM(sizes, dtype)

    gathered = pl.pallas_call(
        exchange_kernel,
        out_shape=(shape(reduced, count), shape(1, count), shape(reduced, count)),
        in_specs=[pl.BlockSpec(memory_space=pltpu.HBM)] * 3,
        out_specs=(vmem,) * 3,
        scratch_shapes=[
            hold(reduced, own), hold(1, own), hold(reduced, own), dma((3,)), dma((3,)), dma((feats, 3)),
        ],
        compiler_params=pltpu.CompilerParams(vmem_limit_bytes=LIMIT, collective_id=1, has_side_effects=True),
        name="exchange",
    )(*[pltpu.with_memory_space_constraint(x, pltpu.HBM) for x in (states, inputs[None], targets)])
    square = shape(count, count)
    short = shape(count, count, dtype=BF16)
    solved = pl.pallas_call(
        inverse_kernel,
        out_shape=(short, short, square, shape(1, LANES)),
        in_specs=[vmem] * 2,
        out_specs=(vmem,) * 4,
        scratch_shapes=[
            hold(count, count), hold(count, count, dtype=BF16),
            hold(count, count, dtype=BF16), hold(count, count, dtype=BF16),
        ],
        compiler_params=pltpu.CompilerParams(vmem_limit_bytes=LIMIT),
        name="local_inverse",
    )(gathered[0], gathered[1])
    block = shape(half, columns)
    first_owners, second_owners, order = choose(spots, owners)
    after, duals, last, history = pl.pallas_call(
        functools.partial(
            second_kernel, width=width, first_owners=first_owners, second_owners=second_owners, order=order
        ),
        out_shape=(block, block, block, shape(4, LANES)),
        in_specs=[vmem] * 7,
        out_specs=(vmem,) * 4,
        scratch_shapes=[
            hold(columns, count),
            hold(columns, count, dtype=BF16), hold(columns, count, dtype=BF16),
            hold(count, columns, dtype=BF16), hold(count, columns, dtype=BF16),
            hold(count, count), hold(count, count, dtype=BF16), hold(count, count, dtype=BF16),
            hold(count, count, dtype=BF16), hold(reduced, count),
            hold(owners, reduced, wide), hold(owners, reduced + 1, wide),
            hold(slabs, reduced, wide), hold(slabs, reduced + 1, wide),
            hold(reduced, wide), hold(feats, half + 4, wide),
            hold(owners, reduced, wide), hold(owners, half + 4, wide),
            hold(2, half, columns), hold(max(feats - 1, 1), 2, half, columns),
            hold(slabs * feats, half + 4, wide),
            dma, dma, dma, dma, dma, dma, dma, dma, dma((max(feats - 1, 1),)), dma,
        ],
        compiler_params=pltpu.CompilerParams(vmem_limit_bytes=2 * LIMIT, collective_id=0, has_side_effects=True),
        name="second_and_averages",
    )(*gathered, *solved)
    shard = shape(half, width)
    spread_rows = shape(half, 1, width)
    after, duals, last, history = pl.pallas_call(
        last_kernel,
        out_shape=(spread_rows, spread_rows, shard, shape(2, 2)),
        in_specs=[vmem] * 4,
        out_specs=(vmem,) * 4,
        compiler_params=pltpu.CompilerParams(vmem_limit_bytes=4 * 2**20),
        name="outputs",
    )(after, duals, last, history)
    return (jnp.swapaxes(after, 0, 1), jnp.swapaxes(duals, 0, 1), last, history)


def choose(spots, owners):
    slabs = range(len(spots))
    apart = [[sum(abs(a - b) for a, b in zip(spots[p], spots[q])) for q in slabs] for p in slabs]
    first = sorted(slabs, key=lambda q: (max(apart[q]), -apart[0][q], q))[:owners]
    second = sorted(slabs, key=lambda q: (max(apart[q]), apart[0][q], q))[:owners]
    return sorted(first), sorted(second), sorted(slabs, key=lambda p: (apart[0][p], p))


def solution(mesh):
    spots = [
        tuple(getattr(device, "coords", None) or (index,)) for index, device in enumerate(mesh.devices[:, 0])
    ]
    in_specs = (P(None, ("slab", "feat")), P(("slab", "feat")), P(None, ("slab", "feat")))
    out_specs = (P("slab", "feat", None), P("slab", "feat", None), P("feat", None), P())
    body = functools.partial(shards, spots=spots)
    return jax.shard_map(body, mesh=mesh, in_specs=in_specs, out_specs=out_specs, check_vma=False)
```

```python
import functools

import jax
import jax.numpy as jnp
from jax import lax
from jax.experimental import pallas as pl
from jax.experimental.pallas import tpu as pltpu
from jax.sharding import PartitionSpec as P

penalty = 1.0
LIMIT = 20 * 2**20
LANES = 128
STEPS = 4
EASY = 400.0
NN = (((1,), (0,)), ((), ()))
NT = (((1,), (1,)), ((), ()))
TN = (((0,), (0,)), ((), ()))
F32 = jnp.float32
BF16 = jnp.bfloat16


def up(value, step):
    return -(-value // step) * step


def dot(left, right, dims=NN):
    return lax.dot_general(left.astype(BF16), right.astype(BF16), dims, preferred_element_type=F32)


def split(value):
    high = value.astype(BF16)
    return high, (value - high.astype(F32)).astype(BF16)


def thin(left, high, low, dims=NN):
    rows = left.shape[0]
    top = left.astype(BF16).astype(F32)
    both = jnp.concatenate([top, left - top], 0).astype(BF16)
    out = dot(both, high, dims) + dot(both, low, dims)
    return out[:rows] + out[rows:]


def eye_mask(size):
    return lax.broadcasted_iota(jnp.int32, (size, size), 0) == lax.broadcasted_iota(jnp.int32, (size, size), 1)


def eye(size):
    return jnp.where(eye_mask(size), 1.0, 0.0)


def less_eye(value, target, part):
    for p in range(0, value.shape[0], LANES):
        for q in range(part.start, part.stop, LANES):
            piece = value[p : p + LANES, q - part.start : q - part.start + LANES]
            piece = piece - eye(LANES) if p == q else piece
            target[p : p + LANES, q : q + LANES] = piece.astype(BF16)


def invert_by_pivots(source, target):
    size = source.shape[0]
    target[...] = source[...]
    sub = lax.broadcasted_iota(jnp.int32, (size, 1), 0)
    lane = lax.broadcasted_iota(jnp.int32, (1, size), 1)

    def step(k, carry):
        row = target[pl.ds(k, 1), :]
        here = lane == k
        pivot = jnp.sum(jnp.where(here, row, 0.0), axis=1, keepdims=True)
        scaled = jnp.where(here, 1.0, row) / pivot
        whole = target[...]
        column = jnp.sum(jnp.where(here, whole, 0.0), axis=1, keepdims=True)
        column = jnp.where(sub == k, -1.0, column)
        kept = jnp.where(here | (sub == k), 0.0, whole)
        target[...] = kept - column * scaled
        return carry

    lax.fori_loop(0, size, step, 0)


def exchange_kernel(
    states, inputs, targets, all_s, all_u, all_t, near_s, near_u, near_t, local, send, recv
):
    feats = lax.axis_size("feat")
    core = lax.axis_index("feat")
    head = feats - 1
    own = states.shape[1]
    sources = (states, inputs, targets)
    nears = (near_s, near_u, near_t)
    alls = (all_s, all_u, all_t)

    def load(i, target):
        return pltpu.make_async_copy(sources[i], target, local.at[i])

    def move(i, f):
        return pltpu.make_async_remote_copy(
            src_ref=nears[i], dst_ref=alls[i].at[:, pl.ds(f * own, own)], send_sem=send.at[i], recv_sem=recv.at[f, i],
            device_id={"feat": head}, device_id_type=pl.DeviceIdType.MESH,
        )

    barrier = pltpu.get_barrier_semaphore()

    def greet(feat):
        pl.semaphore_signal(barrier, inc=1, device_id={"feat": feat}, device_id_type=pl.DeviceIdType.MESH)

    @pl.when(core == head)
    def _():
        for i in range(3):
            load(i, alls[i].at[:, pl.ds(head * own, own)]).start()
        for f in range(head):
            greet(f)
        pl.semaphore_wait(barrier, head)
        for i in range(3):
            load(i, alls[i].at[:, pl.ds(head * own, own)]).wait()
        for f in range(head):
            for i in range(3):
                move(i, f).wait_recv()

    for f in range(head):

        @pl.when(core == f)
        def _():
            for i in range(3):
                load(i, nears[i]).start()
            greet(head)
            pl.semaphore_wait(barrier, 1)
            for i in range(3):
                load(i, nears[i]).wait()
                move(i, f).start()
            for i in range(3):
                move(i, f).wait_send()


def stacked(value, orders):
    parts = []
    rest = value
    for _ in range(1 + max(max(order) for order in orders)):
        high = rest.astype(BF16).astype(F32)
        parts.append(high)
        rest = rest - high
    left = jnp.concatenate([parts[i] for i, _ in orders], 0)
    right = jnp.concatenate([parts[j] for _, j in orders], 0)
    return left.astype(BF16), right.astype(BF16)


def newton_scale(delta):
    return 2.0 / (2.0 - delta * delta), delta * delta / (2.0 - delta * delta)


def inverse_kernel(all_s, all_u, high_a, low_a, start, inverse, info, system, shifted, high_x, low_x):
    reduced, count = all_s.shape
    edge = LANES
    spans = [slice(k, k + edge) for k in range(0, count, edge)]

    def solve():
        s = all_s[...]
        sub = lax.broadcasted_iota(jnp.int32, (8, count), 0)
        last = jnp.where(sub == 0, all_u[...], jnp.where(sub == 1, 1.0, 0.0)) * (1.0 / count) ** 0.5
        left, right = stacked(s * (0.5 / count) ** 0.25, ((0, 0), (0, 1), (1, 0), (0, 2), (2, 0), (1, 1)))
        extra = jnp.concatenate([s * s * (0.5 / count) ** 0.5, last], 0)
        left2, right2 = stacked(extra, ((0, 0), (0, 1), (1, 0)))
        sums = [jnp.zeros((8, edge), F32)] * len(spans)
        for p, down in enumerate(spans):
            inner = dot(left[:, down], right, TN)
            other = dot(left2[:, down], right2, TN)
            for q, across in enumerate(spans):
                part = inner[:, across]
                part = part * (part + (2.0 / count) ** 0.5) + other[:, across]
                if p == q:
                    part = part + jnp.where(eye_mask(edge), penalty, 0.0)
                system[down, across] = part
                high_a[down, across], low_a[down, across] = split(part)
                sums[q] = sums[q] + jnp.abs(part).reshape(edge // 8, 8, edge).sum(0)
        sums = functools.reduce(jnp.maximum, [jnp.sum(part, axis=0, keepdims=True) for part in sums])
        high = jnp.max(sums) / penalty
        delta = (high - 1.0) / (high + 1.0)
        alpha = 2.0 / ((1.0 + high) * penalty)
        c, later = newton_scale(delta)

        def begin(target, dtype):
            for p, down in enumerate(spans):
                for q, across in enumerate(spans):
                    part = (-c * alpha * alpha) * system[down, across]
                    if p == q:
                        part = part + jnp.where(eye_mask(edge), 2.0 * c * alpha, 0.0)
                    target[down, across] = part.astype(dtype)

        begin(start, BF16)
        hard = jnp.logical_not(high <= EASY)
        lane = lax.broadcasted_iota(jnp.int32, (1, LANES), 1)
        info[...] = jnp.where(lane == 0, later, jnp.where(hard, 1.0, 0.0))

        @pl.when(hard)
        def _():
            begin(inverse, F32)
            careful(later)

    def careful(delta):
        sub = lax.broadcasted_iota(jnp.int32, (8, count), 0)
        mixed = (lax.broadcasted_iota(jnp.int32, (8, count), 1) + 1) * (sub * 40503 + 30011)
        mixed = (mixed ^ (mixed >> 7)) * 9973
        signs = jnp.where(((mixed >> 9) & 1) == 1, 1.0, -1.0)

        def coarse(state):
            step, delta = state
            x = inverse[...].astype(BF16)
            shifted[...] = dot(high_a[...], x).astype(BF16)
            c, later = newton_scale(delta)
            inverse[...] = c * (2.0 * inverse[...] - dot(x, shifted[...]))
            return step + 1, later

        lax.while_loop(lambda state: (state[1] > 0.085) & (state[0] < 12), coarse, (0, delta))

        def polish(state):
            step, _ = state
            high_x[...], low_x[...] = split(inverse[...])
            ah, al, xh, xl = high_a[...], low_a[...], high_x[...], low_x[...]
            shifted[...] = (eye(count) - (dot(ah, xh) + (dot(ah, xl) + dot(al, xh)))).astype(BF16)
            once = signs - thin(thin(signs, xh, xl), ah, al)
            twice = once - thin(thin(once, xh, xl), ah, al)
            inverse[...] = inverse[...] + dot(xh, shifted[...])
            return step + 1, jnp.sum(twice * twice) * (1.0 / 8.0)

        _, worst = lax.while_loop(
            lambda state: jnp.logical_not(state[1] < 0.001) & (state[0] < 8), polish, (0, jnp.float32(1e9))
        )

        @pl.when(jnp.logical_not(worst < 0.001))
        def _():
            invert_by_pivots(system, inverse)

    pl.when(lax.axis_index("feat") == lax.axis_size("feat") - 1)(solve)


def feature_steps(all_s, all_u, phi, high_p, low_p):
    reduced, count = all_s.shape

    def first():
        phi[0:reduced, :] = all_s[...]

    def products(i, row):
        phi[row : row + reduced - i, :] = all_s[i : i + 1, :] * all_s[i:reduced, :]

    def ending(row):
        phi[row : row + 1, :] = all_u[...]
        phi[row + 1 : row + 2, :] = jnp.ones((1, count), F32)
        if row + 2 < phi.shape[0]:
            phi[row + 2 :, :] = jnp.zeros((phi.shape[0] - row - 2, count), F32)

    steps = [first]
    row = reduced
    for i in range(reduced):
        steps.append(functools.partial(products, i, row))
        row += reduced - i
    steps.append(functools.partial(ending, row))

    def narrow(rows):
        high_p[rows, :], low_p[rows, :] = split(phi[rows, :])

    for k in range(0, phi.shape[0], LANES):
        steps.append(functools.partial(narrow, slice(k, k + LANES)))
    return steps


def lanes_of(value):
    return jnp.sum(value.reshape(-1, value.shape[-1]), axis=0, keepdims=True)


def second_kernel(
    all_s, all_u, all_t, high_a, low_a, begin, inverse, info, after, duals, last, history,
    phi, high_p, low_p, high_w, low_w, better, high_b, low_b, gap, answer,
    own1, own2, land1, land2, out1, out2, mean1, mean2, mine, ship, span,
    send1, recv1, spread1, got1, send2, recv2, spread2, got2, ship_send, ship_recv,
    *, width, first_owners, second_owners, order,
):
    slabs = lax.axis_size("slab")
    feats = lax.axis_size("feat")
    me = lax.axis_index("slab")
    core = lax.axis_index("feat")
    owners, reduced, wide = own1.shape
    half = reduced // feats
    count = all_s.shape[1]
    head = feats - 1
    leading = core == head
    everyones = sorted(set(first_owners) | set(second_owners))

    def among(slab_list):
        return functools.reduce(jnp.logical_or, [me == slab for slab in slab_list])

    def place_in(slab_list):
        return functools.reduce(lambda a, b: a + b, [jnp.where(me == slab, k, 0) for k, slab in enumerate(slab_list)])

    inside, inside1, inside2 = among(everyones), among(first_owners), among(second_owners)
    spot1, spot2 = place_in(first_owners), place_in(second_owners)

    def copy(source, target, send, recv, slab, feat):
        return pltpu.make_async_remote_copy(
            src_ref=source, dst_ref=target, send_sem=send, recv_sem=recv,
            device_id={"slab": slab, "feat": feat}, device_id_type=pl.DeviceIdType.MESH,
        )

    def arrived(target, size, sem):
        part = target.at[pl.ds(0, size)]
        copy(part, part, sem, sem, me, core).wait_recv()

    def departed(source, size, sem):
        part = source.at[pl.ds(0, size)]
        copy(part, part, sem, sem, me, core).wait_send()

    def each(order, body):
        if len(order) <= 16:
            for d in order:
                body(d)
            return

        def step(d, carry):
            body(d)
            return carry

        lax.fori_loop(min(order), max(order) + 1, step, 0)

    far = sorted(range(1, slabs), key=lambda d: -min(d, slabs - d))

    def slab_of(d):
        return lax.rem(me + d, slabs)

    def split_on(flag, yes, no):
        pl.when(flag)(yes)
        pl.when(jnp.logical_not(flag))(no)

    barrier = pltpu.get_barrier_semaphore()

    def greet(slab, feat):
        pl.semaphore_signal(
            barrier, inc=1, device_id={"slab": slab, "feat": feat}, device_id_type=pl.DeviceIdType.MESH
        )

    @pl.when(leading & inside)
    def _():
        for f in range(feats):
            each(far, lambda d, f=f: greet(slab_of(d), f))
        for f in range(head):
            greet(me, f)

    @pl.when(jnp.logical_not(leading & inside))
    def _():
        for slab in everyones:
            greet(slab, head)

    @pl.when(leading & jnp.logical_not(inside))
    def _():
        for f in range(head):
            greet(me, f)

    @pl.when(jnp.logical_not(leading) & jnp.logical_not(inside))
    def _():
        greet(me, head)

    def scatter(source, landing, send, recv, slab_list):
        for k, slab in enumerate(slab_list):

            @pl.when(me != slab)
            def _():
                copy(source.at[k], landing.at[me], send, recv, slab, head).start()

    def joined(buffer, rows):
        return jnp.concatenate([buffer[k][:rows] for k in range(owners)], 1)

    def owner_first():
        land1[me] = own1[spot1]
        arrived(land1, slabs - 1, recv1)
        out1[...] = land1[...].sum(0) * (1.0 / slabs)
        each(far, lambda d: copy(out1, mean1.at[spot1], spread1, got1, slab_of(d), head).start())
        mean1[spot1] = out1[...]

    def owner_second():
        old = mean1[spot2]
        dual1 = lanes_of(jnp.square(old))
        land2[me] = own2[spot2]
        arrived(land2, slabs - 1, recv2)
        whole = land2[...].sum(0)
        new = whole[:reduced] * (1.0 / slabs)
        primal2 = lanes_of(jnp.square(land2[:, 0:reduced] - new[None]))
        dual2 = lanes_of(jnp.square(new - old))
        scale = slabs * penalty * penalty
        stats = jnp.concatenate([whole[reduced : reduced + 1], primal2, dual1 * scale, dual2 * scale], 0)
        for f in range(feats):
            out2[f, 0:half] = new[f * half : (f + 1) * half]
            out2[f, half : half + 4] = stats

        def one(slab):
            for f in range(feats):

                @pl.when((me != slab) | (f != head))
                def _():
                    copy(out2.at[f], mean2.at[spot2], spread2, got2, slab, f).start()

        for slab in order:
            one(slab)
        mean2[spot2] = out2[head]

    def leader():
        ah, al = high_a[...], low_a[...]
        delta = info[0:1, 0:1]
        kept = info[0:1, 1:2] > 0.5
        middle = up(count // 2, LANES)
        parts = (slice(0, middle), slice(middle, count))
        steps = feature_steps(all_s, all_u, phi, high_p, low_p)
        chunk = -(-len(steps) // (2 * STEPS))
        old, fresh, spare = begin, high_b, low_b
        size = jnp.ones((1, 1), F32)
        for step in range(STEPS):
            c, delta = newton_scale(delta)
            for part in parts:
                gap[:, part] = dot(ah, old[:, part]).astype(BF16)
                for _ in range(min(chunk, len(steps))):
                    steps.pop(0)()
            x = old[...]
            for part in parts:
                value = (2.0 / size) * old[:, part].astype(F32) - dot(x, gap[:, part])
                if step == STEPS - 1:
                    value = value * (c * size * size)
                fresh[:, part] = value.astype(BF16)
            size = c * size * size
            old, fresh, spare = fresh, spare, fresh
        b = all_t[...] * (1.0 / count)
        x = old[...]
        for part in parts:
            less_eye(dot(ah, x[:, part]) + dot(al, x[:, part]), gap, part)
        for part in parts:
            value = x[:, part].astype(F32) - dot(x, gap[:, part])
            better[:, part] = jnp.where(kept, inverse[:, part], value)
        high_b[...], low_b[...] = split(better[...])
        xh, xl = high_b[...], low_b[...]
        y = thin(b, xh, xl)
        y = y + thin(b - thin(y, ah, al), xh, xl)
        y = y + thin(b - thin(y, ah, al), xh, xl)
        answer[...] = y
        start_value = thin(y, high_p[...], low_p[...], NT)
        for k in range(owners):
            own1[k] = start_value[:, k * wide : (k + 1) * wide]
        split_on(
            inside,
            lambda: pl.semaphore_wait(barrier, slabs * feats - 1),
            lambda: pl.semaphore_wait(barrier, len(everyones) + feats - 1),
        )
        scatter(own1, land1, send1, recv1, first_owners)

        for _ in range(2):
            bh, bl = high_b[...], low_b[...]
            for part in parts:
                less_eye(dot(ah, bh[:, part]) + (dot(ah, bl[:, part]) + dot(al, bh[:, part])), gap, part)
            for part in parts:
                better[:, part] = better[:, part] - dot(bh, gap[:, part])
            high_b[...], low_b[...] = split(better[...])
        pl.when(inside1)(owner_first)
        weights = dot(high_b[...], high_p[...], NT) + (
            dot(high_b[...], low_p[...], NT) + dot(low_b[...], high_p[...], NT)
        )
        high_w[...], low_w[...] = split(weights)

        split_on(
            inside1,
            lambda: arrived(mean1, owners - 1, got1),
            lambda: arrived(mean1, owners, got1),
        )
        first = joined(own1, reduced)
        mean = joined(mean1, reduced)
        v = thin(mean, high_p[...], low_p[...]) * (2.0 / (count * penalty)) + answer[...]
        result = first + 2.0 * mean - thin(v, high_w[...], low_w[...])
        primal1 = jnp.sum(jnp.square(first - mean), axis=0, keepdims=True)
        for k in range(owners):
            own2[k, 0:reduced] = result[:, k * wide : (k + 1) * wide]
            own2[k, reduced : reduced + 1] = primal1[:, k * wide : (k + 1) * wide]
        scatter(own2, land2, send2, recv2, second_owners)
        change = (first - mean) + result
        for f in range(head):
            ship[f, 0] = result[f * half : (f + 1) * half]
            ship[f, 1] = change[f * half : (f + 1) * half]
            copy(ship.at[f], mine, ship_send.at[f], ship_recv, me, f).start()
        mine[0] = result[head * half :]
        mine[1] = change[head * half :]
        pl.when(inside2)(owner_second)

        split_on(inside1, lambda: departed(own1, owners - 1, send1), lambda: departed(own1, owners, send1))
        split_on(inside2, lambda: departed(own2, owners - 1, send2), lambda: departed(own2, owners, send2))
        for f in range(head):
            copy(ship.at[f], mine, ship_send.at[f], ship_recv, me, core).wait_send()

    def follower():
        split_on(
            inside,
            lambda: pl.semaphore_wait(barrier, len(everyones)),
            lambda: pl.semaphore_wait(barrier, len(everyones) + 1),
        )
        copy(ship.at[0], mine, ship_send.at[0], ship_recv, me, core).wait_recv()

    split_on(leading, leader, follower)
    split_on(
        leading & inside2,
        lambda: arrived(mean2, owners - 1, got2),
        lambda: arrived(mean2, owners, got2),
    )
    new = joined(mean2, half)
    after[...] = mine[0]
    last[...] = new
    duals[...] = mine[1] - new
    sums = mean2[0][half : half + 4]
    for k in range(1, owners):
        sums = sums + mean2[k][half : half + 4]
    sums = jnp.sum(sums, axis=1, keepdims=True)
    history[...] = jnp.broadcast_to(jnp.sqrt(sums * (1.0 / (slabs * reduced * width))), history.shape)

    @pl.when(leading & inside1)
    def _():
        departed(land1, slabs - 1, spread1)

    @pl.when(leading & inside2)
    def _():
        departed(span, slabs * feats - 1, spread2)


def last_kernel(after, duals, last, history, out_after, out_duals, out_last, out_history):
    half, width = out_last.shape
    for r in range(half):
        out_after[r] = after[r : r + 1, :width]
        out_duals[r] = duals[r : r + 1, :width]
    out_last[...] = last[:, :width]
    for r in range(2):
        out_history[r : r + 1, :] = jnp.concatenate([history[2 * r + k : 2 * r + k + 1, 0:1] for k in range(2)], 1)


def shards(states, inputs, targets, *, spots):
    reduced, own = states.shape
    feats = lax.axis_size("feat")
    slabs = lax.axis_size("slab")
    half = reduced // feats
    width = reduced + reduced * (reduced + 1) // 2 + 2
    count = own * feats
    tiles = up(width, LANES) // LANES
    wide = -(-tiles // slabs) * LANES
    columns = up(width, wide)
    owners = columns // wide
    vmem = pl.BlockSpec(memory_space=pltpu.VMEM)
    dma = pltpu.SemaphoreType.DMA

    def shape(*sizes, dtype=F32):
        return jax.ShapeDtypeStruct(sizes, dtype)

    def hold(*sizes, dtype=F32):
        return pltpu.VMEM(sizes, dtype)

    gathered = pl.pallas_call(
        exchange_kernel,
        out_shape=(shape(reduced, count), shape(1, count), shape(reduced, count)),
        in_specs=[pl.BlockSpec(memory_space=pltpu.HBM)] * 3,
        out_specs=(vmem,) * 3,
        scratch_shapes=[
            hold(reduced, own), hold(1, own), hold(reduced, own), dma((3,)), dma((3,)), dma((feats, 3)),
        ],
        compiler_params=pltpu.CompilerParams(vmem_limit_bytes=LIMIT, collective_id=1, has_side_effects=True),
        name="exchange",
    )(*[pltpu.with_memory_space_constraint(x, pltpu.HBM) for x in (states, inputs[None], targets)])
    square = shape(count, count)
    short = shape(count, count, dtype=BF16)
    solved = pl.pallas_call(
        inverse_kernel,
        out_shape=(short, short, short, square, shape(1, LANES)),
        in_specs=[vmem] * 2,
        out_specs=(vmem,) * 5,
        scratch_shapes=[
            hold(count, count), hold(count, count, dtype=BF16),
            hold(count, count, dtype=BF16), hold(count, count, dtype=BF16),
        ],
        compiler_params=pltpu.CompilerParams(vmem_limit_bytes=LIMIT),
        name="local_inverse",
    )(gathered[0], gathered[1])
    block = shape(half, columns)
    first_owners, second_owners, order = choose(spots, owners)
    after, duals, last, history = pl.pallas_call(
        functools.partial(
            second_kernel, width=width, first_owners=first_owners, second_owners=second_owners, order=order
        ),
        out_shape=(block, block, block, shape(4, LANES)),
        in_specs=[vmem] * 8,
        out_specs=(vmem,) * 4,
        scratch_shapes=[
            hold(columns, count),
            hold(columns, count, dtype=BF16), hold(columns, count, dtype=BF16),
            hold(count, columns, dtype=BF16), hold(count, columns, dtype=BF16),
            hold(count, count), hold(count, count, dtype=BF16), hold(count, count, dtype=BF16),
            hold(count, count, dtype=BF16), hold(reduced, count),
            hold(owners, reduced, wide), hold(owners, reduced + 1, wide),
            hold(slabs, reduced, wide), hold(slabs, reduced + 1, wide),
            hold(reduced, wide), hold(feats, half + 4, wide),
            hold(owners, reduced, wide), hold(owners, half + 4, wide),
            hold(2, half, columns), hold(max(feats - 1, 1), 2, half, columns),
            hold(slabs * feats, half + 4, wide),
            dma, dma, dma, dma, dma, dma, dma, dma, dma((max(feats - 1, 1),)), dma,
        ],
        compiler_params=pltpu.CompilerParams(vmem_limit_bytes=2 * LIMIT, collective_id=0, has_side_effects=True),
        name="second_and_averages",
    )(*gathered, *solved)
    shard = shape(half, width)
    spread_rows = shape(half, 1, width)
    after, duals, last, history = pl.pallas_call(
        last_kernel,
        out_shape=(spread_rows, spread_rows, shard, shape(2, 2)),
        in_specs=[vmem] * 4,
        out_specs=(vmem,) * 4,
        compiler_params=pltpu.CompilerParams(vmem_limit_bytes=4 * 2**20),
        name="outputs",
    )(after, duals, last, history)
    return (jnp.swapaxes(after, 0, 1), jnp.swapaxes(duals, 0, 1), last, history)


def choose(spots, owners):
    slabs = range(len(spots))
    apart = [[sum(abs(a - b) for a, b in zip(spots[p], spots[q])) for q in slabs] for p in slabs]
    first = sorted(slabs, key=lambda q: (max(apart[q]), -apart[0][q], q))[:owners]
    second = sorted(slabs, key=lambda q: (max(apart[q]), apart[0][q], q))[:owners]
    return sorted(first), sorted(second), sorted(slabs, key=lambda p: (apart[0][p], p))


def solution(mesh):
    spots = [
        tuple(getattr(device, "coords", None) or (index,)) for index, device in enumerate(mesh.devices[:, 0])
    ]
    in_specs = (P(None, ("slab", "feat")), P(("slab", "feat")), P(None, ("slab", "feat")))
    out_specs = (P("slab", "feat", None), P("slab", "feat", None), P("feat", None), P())
    body = functools.partial(shards, spots=spots)
    return jax.shard_map(body, mesh=mesh, in_specs=in_specs, out_specs=out_specs, check_vma=False)
```

```python
import functools

import jax
import jax.numpy as jnp
from jax import lax
from jax.experimental import pallas as pl
from jax.experimental.pallas import tpu as pltpu
from jax.sharding import PartitionSpec as P

penalty = 1.0
LIMIT = 20 * 2**20
LANES = 128
STEPS = 4
EASY = 400.0
NN = (((1,), (0,)), ((), ()))
NT = (((1,), (1,)), ((), ()))
TN = (((0,), (0,)), ((), ()))
F32 = jnp.float32
BF16 = jnp.bfloat16


def up(value, step):
    return -(-value // step) * step


def dot(left, right, dims=NN):
    return lax.dot_general(left.astype(BF16), right.astype(BF16), dims, preferred_element_type=F32)


def split(value):
    high = value.astype(BF16)
    return high, (value - high.astype(F32)).astype(BF16)


def thin(left, high, low, dims=NN):
    rows = left.shape[0]
    top = left.astype(BF16).astype(F32)
    both = jnp.concatenate([top, left - top], 0).astype(BF16)
    out = dot(both, high, dims) + dot(both, low, dims)
    return out[:rows] + out[rows:]


def eye_mask(size):
    return lax.broadcasted_iota(jnp.int32, (size, size), 0) == lax.broadcasted_iota(jnp.int32, (size, size), 1)


def eye(size):
    return jnp.where(eye_mask(size), 1.0, 0.0)


def less_eye(value, target, part):
    for p in range(0, value.shape[0], LANES):
        for q in range(part.start, part.stop, LANES):
            piece = value[p : p + LANES, q - part.start : q - part.start + LANES]
            piece = piece - eye(LANES) if p == q else piece
            target[p : p + LANES, q : q + LANES] = piece.astype(BF16)


def invert_by_pivots(source, target):
    size = source.shape[0]
    target[...] = source[...]
    sub = lax.broadcasted_iota(jnp.int32, (size, 1), 0)
    lane = lax.broadcasted_iota(jnp.int32, (1, size), 1)

    def step(k, carry):
        row = target[pl.ds(k, 1), :]
        here = lane == k
        pivot = jnp.sum(jnp.where(here, row, 0.0), axis=1, keepdims=True)
        scaled = jnp.where(here, 1.0, row) / pivot
        whole = target[...]
        column = jnp.sum(jnp.where(here, whole, 0.0), axis=1, keepdims=True)
        column = jnp.where(sub == k, -1.0, column)
        kept = jnp.where(here | (sub == k), 0.0, whole)
        target[...] = kept - column * scaled
        return carry

    lax.fori_loop(0, size, step, 0)


def exchange_kernel(states, inputs, targets, all_s, all_u, all_t, local, send, recv):
    feats = lax.axis_size("feat")
    core = lax.axis_index("feat")
    head = feats - 1
    own = states.shape[1]
    sources = (states, inputs, targets)
    alls = (all_s, all_u, all_t)

    def load(i):
        return pltpu.make_async_copy(sources[i], alls[i].at[:, pl.ds(head * own, own)], local.at[i])

    def move(i, f):
        return pltpu.make_async_remote_copy(
            src_ref=sources[i], dst_ref=alls[i].at[:, pl.ds(f * own, own)],
            send_sem=send.at[i], recv_sem=recv.at[f, i],
            device_id={"feat": head}, device_id_type=pl.DeviceIdType.MESH,
        )

    barrier = pltpu.get_barrier_semaphore()

    def greet(feat):
        pl.semaphore_signal(barrier, inc=1, device_id={"feat": feat}, device_id_type=pl.DeviceIdType.MESH)

    @pl.when(core == head)
    def _():
        for f in range(head):
            greet(f)
        for i in range(3):
            load(i).start()
        pl.semaphore_wait(barrier, head)
        for i in range(3):
            load(i).wait()
        for f in range(head):
            for i in range(3):
                move(i, f).wait_recv()

    for f in range(head):

        @pl.when(core == f)
        def _():
            greet(head)
            pl.semaphore_wait(barrier, 1)
            for i in range(3):
                move(i, f).start()
            for i in range(3):
                move(i, f).wait_send()


def stacked(value, orders):
    parts = []
    rest = value
    for _ in range(1 + max(max(order) for order in orders)):
        high = rest.astype(BF16).astype(F32)
        parts.append(high)
        rest = rest - high
    left = jnp.concatenate([parts[i] for i, _ in orders], 0)
    right = jnp.concatenate([parts[j] for _, j in orders], 0)
    return left.astype(BF16), right.astype(BF16)


def newton_scale(delta):
    return 2.0 / (2.0 - delta * delta), delta * delta / (2.0 - delta * delta)


def inverse_kernel(all_s, all_u, high_a, low_a, start, inverse, info, system, shifted, high_x, low_x):
    reduced, count = all_s.shape
    edge = LANES
    spans = [slice(k, k + edge) for k in range(0, count, edge)]

    def solve():
        s = all_s[...]
        sub = lax.broadcasted_iota(jnp.int32, (8, count), 0)
        last = jnp.where(sub == 0, all_u[...], jnp.where(sub == 1, 1.0, 0.0)) * (1.0 / count) ** 0.5
        left, right = stacked(s * (0.5 / count) ** 0.25, ((0, 0), (0, 1), (1, 0), (0, 2), (2, 0), (1, 1)))
        extra = jnp.concatenate([s * s * (0.5 / count) ** 0.5, last], 0)
        left2, right2 = stacked(extra, ((0, 0), (0, 1), (1, 0)))
        sums = [jnp.zeros((8, edge), F32)] * len(spans)
        for p, down in enumerate(spans):
            inner = dot(left[:, down], right, TN)
            other = dot(left2[:, down], right2, TN)
            for q, across in enumerate(spans):
                part = inner[:, across]
                part = part * (part + (2.0 / count) ** 0.5) + other[:, across]
                if p == q:
                    part = part + jnp.where(eye_mask(edge), penalty, 0.0)
                system[down, across] = part
                high_a[down, across], low_a[down, across] = split(part)
                sums[q] = sums[q] + jnp.abs(part).reshape(edge // 8, 8, edge).sum(0)
        sums = functools.reduce(jnp.maximum, [jnp.sum(part, axis=0, keepdims=True) for part in sums])
        high = jnp.max(sums) / penalty
        delta = (high - 1.0) / (high + 1.0)
        alpha = 2.0 / ((1.0 + high) * penalty)
        c, later = newton_scale(delta)

        def begin(target, dtype):
            for p, down in enumerate(spans):
                for q, across in enumerate(spans):
                    part = (-c * alpha * alpha) * system[down, across]
                    if p == q:
                        part = part + jnp.where(eye_mask(edge), 2.0 * c * alpha, 0.0)
                    target[down, across] = part.astype(dtype)

        begin(start, BF16)
        hard = jnp.logical_not(high <= EASY)
        lane = lax.broadcasted_iota(jnp.int32, (1, LANES), 1)
        info[...] = jnp.where(lane == 0, later, jnp.where(hard, 1.0, 0.0))

        @pl.when(hard)
        def _():
            begin(inverse, F32)
            careful(later)

    def careful(delta):
        sub = lax.broadcasted_iota(jnp.int32, (8, count), 0)
        mixed = (lax.broadcasted_iota(jnp.int32, (8, count), 1) + 1) * (sub * 40503 + 30011)
        mixed = (mixed ^ (mixed >> 7)) * 9973
        signs = jnp.where(((mixed >> 9) & 1) == 1, 1.0, -1.0)

        def coarse(state):
            step, delta = state
            x = inverse[...].astype(BF16)
            shifted[...] = dot(high_a[...], x).astype(BF16)
            c, later = newton_scale(delta)
            inverse[...] = c * (2.0 * inverse[...] - dot(x, shifted[...]))
            return step + 1, later

        lax.while_loop(lambda state: (state[1] > 0.085) & (state[0] < 12), coarse, (0, delta))

        def polish(state):
            step, _ = state
            high_x[...], low_x[...] = split(inverse[...])
            ah, al, xh, xl = high_a[...], low_a[...], high_x[...], low_x[...]
            shifted[...] = (eye(count) - (dot(ah, xh) + (dot(ah, xl) + dot(al, xh)))).astype(BF16)
            once = signs - thin(thin(signs, xh, xl), ah, al)
            twice = once - thin(thin(once, xh, xl), ah, al)
            inverse[...] = inverse[...] + dot(xh, shifted[...])
            return step + 1, jnp.sum(twice * twice) * (1.0 / 8.0)

        _, worst = lax.while_loop(
            lambda state: jnp.logical_not(state[1] < 0.001) & (state[0] < 8), polish, (0, jnp.float32(1e9))
        )

        @pl.when(jnp.logical_not(worst < 0.001))
        def _():
            invert_by_pivots(system, inverse)

    pl.when(lax.axis_index("feat") == lax.axis_size("feat") - 1)(solve)


def feature_steps(all_s, all_u, phi, high_p, low_p):
    reduced, count = all_s.shape

    def first():
        phi[0:reduced, :] = all_s[...]

    def products(i, row):
        phi[row : row + reduced - i, :] = all_s[i : i + 1, :] * all_s[i:reduced, :]

    def ending(row):
        phi[row : row + 1, :] = all_u[...]
        phi[row + 1 : row + 2, :] = jnp.ones((1, count), F32)
        if row + 2 < phi.shape[0]:
            phi[row + 2 :, :] = jnp.zeros((phi.shape[0] - row - 2, count), F32)

    steps = [first]
    row = reduced
    for i in range(reduced):
        steps.append(functools.partial(products, i, row))
        row += reduced - i
    steps.append(functools.partial(ending, row))

    def narrow(rows):
        high_p[rows, :], low_p[rows, :] = split(phi[rows, :])

    for k in range(0, phi.shape[0], LANES):
        steps.append(functools.partial(narrow, slice(k, k + LANES)))
    return steps


def lanes_of(value):
    return jnp.sum(value.reshape(-1, value.shape[-1]), axis=0, keepdims=True)


def second_kernel(
    all_s, all_u, all_t, high_a, low_a, begin, inverse, info, after, duals, last, history,
    phi, high_p, low_p, high_w, low_w, better, high_b, low_b, gap, answer,
    own1, own2, land1, land2, out1, out2, mean1, mean2, mine, ship, span,
    send1, recv1, spread1, got1, send2, recv2, spread2, got2, ship_send, ship_recv,
    *, width, first_owners, second_owners, order,
):
    slabs = lax.axis_size("slab")
    feats = lax.axis_size("feat")
    me = lax.axis_index("slab")
    core = lax.axis_index("feat")
    owners, reduced, wide = own1.shape
    half = reduced // feats
    count = all_s.shape[1]
    head = feats - 1
    leading = core == head
    everyones = sorted(set(first_owners) | set(second_owners))

    def among(slab_list):
        return functools.reduce(jnp.logical_or, [me == slab for slab in slab_list])

    def place_in(slab_list):
        return functools.reduce(lambda a, b: a + b, [jnp.where(me == slab, k, 0) for k, slab in enumerate(slab_list)])

    inside, inside1, inside2 = among(everyones), among(first_owners), among(second_owners)
    spot1, spot2 = place_in(first_owners), place_in(second_owners)

    def copy(source, target, send, recv, slab, feat):
        return pltpu.make_async_remote_copy(
            src_ref=source, dst_ref=target, send_sem=send, recv_sem=recv,
            device_id={"slab": slab, "feat": feat}, device_id_type=pl.DeviceIdType.MESH,
        )

    def arrived(target, size, sem):
        part = target.at[pl.ds(0, size)]
        copy(part, part, sem, sem, me, core).wait_recv()

    def departed(source, size, sem):
        part = source.at[pl.ds(0, size)]
        copy(part, part, sem, sem, me, core).wait_send()

    def each(order, body):
        if len(order) <= 16:
            for d in order:
                body(d)
            return

        def step(d, carry):
            body(d)
            return carry

        lax.fori_loop(min(order), max(order) + 1, step, 0)

    far = sorted(range(1, slabs), key=lambda d: -min(d, slabs - d))

    def slab_of(d):
        return lax.rem(me + d, slabs)

    def split_on(flag, yes, no):
        pl.when(flag)(yes)
        pl.when(jnp.logical_not(flag))(no)

    barrier = pltpu.get_barrier_semaphore()

    def greet(slab, feat):
        pl.semaphore_signal(
            barrier, inc=1, device_id={"slab": slab, "feat": feat}, device_id_type=pl.DeviceIdType.MESH
        )

    @pl.when(leading & inside)
    def _():
        for f in range(feats):
            each(far, lambda d, f=f: greet(slab_of(d), f))
        for f in range(head):
            greet(me, f)

    @pl.when(jnp.logical_not(leading & inside))
    def _():
        for slab in everyones:
            greet(slab, head)

    @pl.when(leading & jnp.logical_not(inside))
    def _():
        for f in range(head):
            greet(me, f)

    @pl.when(jnp.logical_not(leading) & jnp.logical_not(inside))
    def _():
        greet(me, head)

    def scatter(source, landing, send, recv, slab_list, group):
        for k, slab in enumerate(slab_list):
            if k not in group:
                continue

            @pl.when(me != slab)
            def _():
                copy(source.at[k], landing.at[me], send, recv, slab, head).start()

    def joined(buffer, rows):
        return jnp.concatenate([buffer[k][:rows] for k in range(owners)], 1)

    def owner_first():
        land1[me] = own1[spot1]
        arrived(land1, slabs - 1, recv1)
        out1[...] = land1[...].sum(0) * (1.0 / slabs)
        each(far, lambda d: copy(out1, mean1.at[spot1], spread1, got1, slab_of(d), head).start())
        mean1[spot1] = out1[...]

    def owner_second():
        old = mean1[spot2]
        dual1 = lanes_of(jnp.square(old))
        land2[me] = own2[spot2]
        arrived(land2, slabs - 1, recv2)
        whole = land2[...].sum(0)
        new = whole[:reduced] * (1.0 / slabs)
        primal2 = lanes_of(jnp.square(land2[:, 0:reduced] - new[None]))
        dual2 = lanes_of(jnp.square(new - old))
        scale = slabs * penalty * penalty
        stats = jnp.concatenate([whole[reduced : reduced + 1], primal2, dual1 * scale, dual2 * scale], 0)
        for f in range(feats):
            out2[f, 0:half] = new[f * half : (f + 1) * half]
            out2[f, half : half + 4] = stats

        def one(slab):
            for f in range(feats):

                @pl.when((me != slab) | (f != head))
                def _():
                    copy(out2.at[f], mean2.at[spot2], spread2, got2, slab, f).start()

        for slab in order:
            one(slab)
        mean2[spot2] = out2[head]

    near_half = -(-owners // 2)
    groups = (range(0, near_half), range(near_half, owners))

    def leader():
        ah, al = high_a[...], low_a[...]
        delta = info[0:1, 0:1]
        kept = info[0:1, 1:2] > 0.5
        middle = up(count // 2, LANES)
        parts = (slice(0, middle), slice(middle, count))
        steps = feature_steps(all_s, all_u, phi, high_p, low_p)
        chunk = -(-len(steps) // (2 * STEPS))
        old, fresh, spare = begin, high_b, low_b
        size = jnp.ones((1, 1), F32)
        for step in range(STEPS):
            c, delta = newton_scale(delta)
            for part in parts:
                gap[:, part] = dot(ah, old[:, part]).astype(BF16)
                for _ in range(min(chunk, len(steps))):
                    steps.pop(0)()
            x = old[...]
            for part in parts:
                value = (2.0 / size) * old[:, part].astype(F32) - dot(x, gap[:, part])
                if step == STEPS - 1:
                    value = value * (c * size * size)
                fresh[:, part] = value.astype(BF16)
            size = c * size * size
            old, fresh, spare = fresh, spare, fresh
        b = all_t[...] * (1.0 / count)
        x = old[...]
        for part in parts:
            less_eye(dot(ah, x[:, part]) + dot(al, x[:, part]), gap, part)
        for part in parts:
            value = x[:, part].astype(F32) - dot(x, gap[:, part])
            better[:, part] = jnp.where(kept, inverse[:, part], value)
        high_b[...], low_b[...] = split(better[...])
        xh, xl = high_b[...], low_b[...]
        y = thin(b, xh, xl)
        y = y + thin(b - thin(y, ah, al), xh, xl)
        y = y + thin(b - thin(y, ah, al), xh, xl)
        answer[...] = y
        for group in groups:
            across = slice(group.start * wide, group.stop * wide)
            start_value = thin(y, high_p[across, :], low_p[across, :], NT)
            for k in group:
                near = (k - group.start) * wide
                own1[k] = start_value[:, near : near + wide]
            if group is groups[0]:
                split_on(
                    inside,
                    lambda: pl.semaphore_wait(barrier, slabs * feats - 1),
                    lambda: pl.semaphore_wait(barrier, len(everyones) + feats - 1),
                )
            scatter(own1, land1, send1, recv1, first_owners, group)

        for _ in range(2):
            bh, bl = high_b[...], low_b[...]
            for part in parts:
                less_eye(dot(ah, bh[:, part]) + (dot(ah, bl[:, part]) + dot(al, bh[:, part])), gap, part)
            for part in parts:
                better[:, part] = better[:, part] - dot(bh, gap[:, part])
            high_b[...], low_b[...] = split(better[...])
        pl.when(inside1)(owner_first)
        weights = dot(high_b[...], high_p[...], NT) + (
            dot(high_b[...], low_p[...], NT) + dot(low_b[...], high_p[...], NT)
        )
        high_w[...], low_w[...] = split(weights)

        split_on(
            inside1,
            lambda: arrived(mean1, owners - 1, got1),
            lambda: arrived(mean1, owners, got1),
        )
        first = joined(own1, reduced)
        mean = joined(mean1, reduced)
        v = thin(mean, high_p[...], low_p[...]) * (2.0 / (count * penalty)) + answer[...]
        primal1 = jnp.sum(jnp.square(first - mean), axis=0, keepdims=True)
        results = []
        for group in groups:
            across = slice(group.start * wide, group.stop * wide)
            result = first[:, across] + 2.0 * mean[:, across] - thin(v, high_w[:, across], low_w[:, across])
            for k in group:
                near = (k - group.start) * wide
                own2[k, 0:reduced] = result[:, near : near + wide]
                own2[k, reduced : reduced + 1] = primal1[:, k * wide : (k + 1) * wide]
            scatter(own2, land2, send2, recv2, second_owners, group)
            results.append(result)
        result = jnp.concatenate(results, 1)
        change = (first - mean) + result
        for f in range(head):
            ship[f, 0] = result[f * half : (f + 1) * half]
            ship[f, 1] = change[f * half : (f + 1) * half]
            copy(ship.at[f], mine, ship_send.at[f], ship_recv, me, f).start()
        mine[0] = result[head * half :]
        mine[1] = change[head * half :]
        pl.when(inside2)(owner_second)

        split_on(inside1, lambda: departed(own1, owners - 1, send1), lambda: departed(own1, owners, send1))
        split_on(inside2, lambda: departed(own2, owners - 1, send2), lambda: departed(own2, owners, send2))
        for f in range(head):
            copy(ship.at[f], mine, ship_send.at[f], ship_recv, me, core).wait_send()

    def follower():
        split_on(
            inside,
            lambda: pl.semaphore_wait(barrier, len(everyones)),
            lambda: pl.semaphore_wait(barrier, len(everyones) + 1),
        )
        copy(ship.at[0], mine, ship_send.at[0], ship_recv, me, core).wait_recv()

    split_on(leading, leader, follower)
    split_on(
        leading & inside2,
        lambda: arrived(mean2, owners - 1, got2),
        lambda: arrived(mean2, owners, got2),
    )
    new = joined(mean2, half)
    after[...] = mine[0]
    last[...] = new
    duals[...] = mine[1] - new
    sums = mean2[0][half : half + 4]
    for k in range(1, owners):
        sums = sums + mean2[k][half : half + 4]
    sums = jnp.sum(sums, axis=1, keepdims=True)
    history[...] = jnp.broadcast_to(jnp.sqrt(sums * (1.0 / (slabs * reduced * width))), history.shape)

    @pl.when(leading & inside1)
    def _():
        departed(land1, slabs - 1, spread1)

    @pl.when(leading & inside2)
    def _():
        departed(span, slabs * feats - 1, spread2)


def last_kernel(after, duals, last, history, out_after, out_duals, out_last, out_history):
    half, width = out_last.shape
    for r in range(half):
        out_after[r] = after[r : r + 1, :width]
        out_duals[r] = duals[r : r + 1, :width]
    out_last[...] = last[:, :width]
    for r in range(2):
        out_history[r : r + 1, :] = jnp.concatenate([history[2 * r + k : 2 * r + k + 1, 0:1] for k in range(2)], 1)


def shards(states, inputs, targets, *, spots):
    reduced, own = states.shape
    feats = lax.axis_size("feat")
    slabs = lax.axis_size("slab")
    half = reduced // feats
    width = reduced + reduced * (reduced + 1) // 2 + 2
    count = own * feats
    tiles = up(width, LANES) // LANES
    wide = -(-tiles // slabs) * LANES
    columns = up(width, wide)
    owners = columns // wide
    vmem = pl.BlockSpec(memory_space=pltpu.VMEM)
    dma = pltpu.SemaphoreType.DMA

    def shape(*sizes, dtype=F32):
        return jax.ShapeDtypeStruct(sizes, dtype)

    def hold(*sizes, dtype=F32):
        return pltpu.VMEM(sizes, dtype)

    gathered = pl.pallas_call(
        exchange_kernel,
        out_shape=(shape(reduced, count), shape(1, count), shape(reduced, count)),
        in_specs=[pl.BlockSpec(memory_space=pltpu.HBM)] * 3,
        out_specs=(vmem,) * 3,
        scratch_shapes=[dma((3,)), dma((3,)), dma((feats, 3))],
        compiler_params=pltpu.CompilerParams(vmem_limit_bytes=LIMIT, collective_id=1, has_side_effects=True),
        name="exchange",
    )(*[pltpu.with_memory_space_constraint(x, pltpu.HBM) for x in (states, inputs[None], targets)])
    square = shape(count, count)
    short = shape(count, count, dtype=BF16)
    solved = pl.pallas_call(
        inverse_kernel,
        out_shape=(short, short, short, square, shape(1, LANES)),
        in_specs=[vmem] * 2,
        out_specs=(vmem,) * 5,
        scratch_shapes=[
            hold(count, count), hold(count, count, dtype=BF16),
            hold(count, count, dtype=BF16), hold(count, count, dtype=BF16),
        ],
        compiler_params=pltpu.CompilerParams(vmem_limit_bytes=LIMIT),
        name="local_inverse",
    )(gathered[0], gathered[1])
    block = shape(half, columns)
    first_owners, second_owners, order = choose(spots, owners)
    after, duals, last, history = pl.pallas_call(
        functools.partial(
            second_kernel, width=width, first_owners=first_owners, second_owners=second_owners, order=order
        ),
        out_shape=(block, block, block, shape(4, LANES)),
        in_specs=[vmem] * 8,
        out_specs=(vmem,) * 4,
        scratch_shapes=[
            hold(columns, count),
            hold(columns, count, dtype=BF16), hold(columns, count, dtype=BF16),
            hold(count, columns, dtype=BF16), hold(count, columns, dtype=BF16),
            hold(count, count), hold(count, count, dtype=BF16), hold(count, count, dtype=BF16),
            hold(count, count, dtype=BF16), hold(reduced, count),
            hold(owners, reduced, wide), hold(owners, reduced + 1, wide),
            hold(slabs, reduced, wide), hold(slabs, reduced + 1, wide),
            hold(reduced, wide), hold(feats, half + 4, wide),
            hold(owners, reduced, wide), hold(owners, half + 4, wide),
            hold(2, half, columns), hold(max(feats - 1, 1), 2, half, columns),
            hold(slabs * feats, half + 4, wide),
            dma, dma, dma, dma, dma, dma, dma, dma, dma((max(feats - 1, 1),)), dma,
        ],
        compiler_params=pltpu.CompilerParams(vmem_limit_bytes=2 * LIMIT, collective_id=0, has_side_effects=True),
        name="second_and_averages",
    )(*gathered, *solved)
    shard = shape(half, width)
    spread_rows = shape(half, 1, width)
    after, duals, last, history = pl.pallas_call(
        last_kernel,
        out_shape=(spread_rows, spread_rows, shard, shape(2, 2)),
        in_specs=[vmem] * 4,
        out_specs=(vmem,) * 4,
        compiler_params=pltpu.CompilerParams(vmem_limit_bytes=4 * 2**20),
        name="outputs",
    )(after, duals, last, history)
    return (jnp.swapaxes(after, 0, 1), jnp.swapaxes(duals, 0, 1), last, history)


def choose(spots, owners):
    slabs = range(len(spots))
    apart = [[sum(abs(a - b) for a, b in zip(spots[p], spots[q])) for q in slabs] for p in slabs]
    first = sorted(slabs, key=lambda q: (max(apart[q]), -apart[0][q], q))[:owners]
    second = sorted(slabs, key=lambda q: (max(apart[q]), apart[0][q], q))[:owners]
    return sorted(first), sorted(second), sorted(slabs, key=lambda p: (apart[0][p], p))


def solution(mesh):
    spots = [
        tuple(getattr(device, "coords", None) or (index,)) for index, device in enumerate(mesh.devices[:, 0])
    ]
    in_specs = (P(None, ("slab", "feat")), P(("slab", "feat")), P(None, ("slab", "feat")))
    out_specs = (P("slab", "feat", None), P("slab", "feat", None), P("feat", None), P())
    body = functools.partial(shards, spots=spots)
    return jax.shard_map(body, mesh=mesh, in_specs=in_specs, out_specs=out_specs, check_vma=False)
```

```python
import functools

import jax
import jax.numpy as jnp
from jax import lax
from jax.experimental import pallas as pl
from jax.experimental.pallas import tpu as pltpu
from jax.sharding import PartitionSpec as P

penalty = 1.0
LIMIT = 20 * 2**20
LANES = 128
STEPS = 3
EASY = 200.0
NN = (((1,), (0,)), ((), ()))
NT = (((1,), (1,)), ((), ()))
TN = (((0,), (0,)), ((), ()))
F32 = jnp.float32
BF16 = jnp.bfloat16


def up(value, step):
    return -(-value // step) * step


def dot(left, right, dims=NN):
    return lax.dot_general(left.astype(BF16), right.astype(BF16), dims, preferred_element_type=F32)


def split(value):
    high = value.astype(BF16)
    return high, (value - high.astype(F32)).astype(BF16)


def thin(left, high, low, dims=NN):
    rows = left.shape[0]
    top = left.astype(BF16).astype(F32)
    both = jnp.concatenate([top, left - top], 0).astype(BF16)
    out = dot(both, high, dims) + dot(both, low, dims)
    return out[:rows] + out[rows:]


def eye_mask(size):
    return lax.broadcasted_iota(jnp.int32, (size, size), 0) == lax.broadcasted_iota(jnp.int32, (size, size), 1)


def eye(size):
    return jnp.where(eye_mask(size), 1.0, 0.0)


def less_eye(value, target, part):
    for p in range(0, value.shape[0], LANES):
        for q in range(part.start, part.stop, LANES):
            piece = value[p : p + LANES, q - part.start : q - part.start + LANES]
            piece = piece - eye(LANES) if p == q else piece
            target[p : p + LANES, q : q + LANES] = piece.astype(BF16)


def invert_by_pivots(source, target):
    size = source.shape[0]
    target[...] = source[...]
    sub = lax.broadcasted_iota(jnp.int32, (size, 1), 0)
    lane = lax.broadcasted_iota(jnp.int32, (1, size), 1)

    def step(k, carry):
        row = target[pl.ds(k, 1), :]
        here = lane == k
        pivot = jnp.sum(jnp.where(here, row, 0.0), axis=1, keepdims=True)
        scaled = jnp.where(here, 1.0, row) / pivot
        whole = target[...]
        column = jnp.sum(jnp.where(here, whole, 0.0), axis=1, keepdims=True)
        column = jnp.where(sub == k, -1.0, column)
        kept = jnp.where(here | (sub == k), 0.0, whole)
        target[...] = kept - column * scaled
        return carry

    lax.fori_loop(0, size, step, 0)


def exchange_kernel(states, inputs, targets, all_s, all_u, all_t, local, send, recv):
    feats = lax.axis_size("feat")
    core = lax.axis_index("feat")
    head = feats - 1
    own = states.shape[1]
    sources = (states, inputs, targets)
    alls = (all_s, all_u, all_t)

    def load(i):
        return pltpu.make_async_copy(sources[i], alls[i].at[:, pl.ds(head * own, own)], local.at[i])

    def move(i, f):
        return pltpu.make_async_remote_copy(
            src_ref=sources[i], dst_ref=alls[i].at[:, pl.ds(f * own, own)],
            send_sem=send.at[i], recv_sem=recv.at[f, i],
            device_id={"feat": head}, device_id_type=pl.DeviceIdType.MESH,
        )

    barrier = pltpu.get_barrier_semaphore()

    def greet(feat):
        pl.semaphore_signal(barrier, inc=1, device_id={"feat": feat}, device_id_type=pl.DeviceIdType.MESH)

    @pl.when(core == head)
    def _():
        for f in range(head):
            greet(f)
        for i in range(3):
            load(i).start()
        pl.semaphore_wait(barrier, head)
        for i in range(3):
            load(i).wait()
        for f in range(head):
            for i in range(3):
                move(i, f).wait_recv()

    for f in range(head):

        @pl.when(core == f)
        def _():
            greet(head)
            pl.semaphore_wait(barrier, 1)
            for i in range(3):
                move(i, f).start()
            for i in range(3):
                move(i, f).wait_send()


def stacked(value, orders):
    parts = []
    rest = value
    for _ in range(1 + max(max(order) for order in orders)):
        high = rest.astype(BF16).astype(F32)
        parts.append(high)
        rest = rest - high
    left = jnp.concatenate([parts[i] for i, _ in orders], 0)
    right = jnp.concatenate([parts[j] for _, j in orders], 0)
    return left.astype(BF16), right.astype(BF16)


def newton_scale(delta):
    return 2.0 / (2.0 - delta * delta), delta * delta / (2.0 - delta * delta)


def inverse_kernel(all_s, all_u, high_a, low_a, start, inverse, info, system, shifted, high_x, low_x):
    reduced, count = all_s.shape
    edge = LANES
    spans = [slice(k, k + edge) for k in range(0, count, edge)]

    def solve():
        s = all_s[...]
        sub = lax.broadcasted_iota(jnp.int32, (8, count), 0)
        last = jnp.where(sub == 0, all_u[...], jnp.where(sub == 1, 1.0, 0.0)) * (1.0 / count) ** 0.5
        left, right = stacked(s * (0.5 / count) ** 0.25, ((0, 0), (0, 1), (1, 0), (0, 2), (2, 0), (1, 1)))
        extra = jnp.concatenate([s * s * (0.5 / count) ** 0.5, last], 0)
        left2, right2 = stacked(extra, ((0, 0), (0, 1), (1, 0)))
        sums = [jnp.zeros((8, edge), F32)] * len(spans)
        for p, down in enumerate(spans):
            inner = dot(left[:, down], right, TN)
            other = dot(left2[:, down], right2, TN)
            for q, across in enumerate(spans):
                part = inner[:, across]
                part = part * (part + (2.0 / count) ** 0.5) + other[:, across]
                if p == q:
                    part = part + jnp.where(eye_mask(edge), penalty, 0.0)
                system[down, across] = part
                high_a[down, across], low_a[down, across] = split(part)
                size = jnp.abs(part)
                shifted[down, across] = size.astype(BF16)
                sums[q] = sums[q] + size.reshape(edge // 8, 8, edge).sum(0)
        sums = jnp.concatenate([jnp.broadcast_to(jnp.sum(part, axis=0, keepdims=True), (8, edge)) for part in sums], 1)
        trial = sums.astype(BF16)
        high = jnp.max(dot(trial, shifted[...]) / trial.astype(F32)) * (1.005 / penalty)
        delta = (high - 1.0) / (high + 1.0)
        alpha = 2.0 / ((1.0 + high) * penalty)
        c, later = newton_scale(delta)

        def begin(target, dtype):
            for p, down in enumerate(spans):
                for q, across in enumerate(spans):
                    part = (-c * alpha * alpha) * system[down, across]
                    if p == q:
                        part = part + jnp.where(eye_mask(edge), 2.0 * c * alpha, 0.0)
                    target[down, across] = part.astype(dtype)

        begin(start, BF16)
        hard = jnp.logical_not(high <= EASY)
        lane = lax.broadcasted_iota(jnp.int32, (1, LANES), 1)
        info[...] = jnp.where(lane == 0, later, jnp.where(hard, 1.0, 0.0))

        @pl.when(hard)
        def _():
            begin(inverse, F32)
            careful(later)

    def careful(delta):
        sub = lax.broadcasted_iota(jnp.int32, (8, count), 0)
        mixed = (lax.broadcasted_iota(jnp.int32, (8, count), 1) + 1) * (sub * 40503 + 30011)
        mixed = (mixed ^ (mixed >> 7)) * 9973
        signs = jnp.where(((mixed >> 9) & 1) == 1, 1.0, -1.0)

        def coarse(state):
            step, delta = state
            x = inverse[...].astype(BF16)
            shifted[...] = dot(high_a[...], x).astype(BF16)
            c, later = newton_scale(delta)
            inverse[...] = c * (2.0 * inverse[...] - dot(x, shifted[...]))
            return step + 1, later

        lax.while_loop(lambda state: (state[1] > 0.085) & (state[0] < 12), coarse, (0, delta))

        def polish(state):
            step, _ = state
            high_x[...], low_x[...] = split(inverse[...])
            ah, al, xh, xl = high_a[...], low_a[...], high_x[...], low_x[...]
            shifted[...] = (eye(count) - (dot(ah, xh) + (dot(ah, xl) + dot(al, xh)))).astype(BF16)
            once = signs - thin(thin(signs, xh, xl), ah, al)
            twice = once - thin(thin(once, xh, xl), ah, al)
            inverse[...] = inverse[...] + dot(xh, shifted[...])
            return step + 1, jnp.sum(twice * twice) * (1.0 / 8.0)

        _, worst = lax.while_loop(
            lambda state: jnp.logical_not(state[1] < 0.001) & (state[0] < 8), polish, (0, jnp.float32(1e9))
        )

        @pl.when(jnp.logical_not(worst < 0.001))
        def _():
            invert_by_pivots(system, inverse)

    pl.when(lax.axis_index("feat") == lax.axis_size("feat") - 1)(solve)


def feature_steps(all_s, all_u, phi, high_p, low_p):
    reduced, count = all_s.shape

    def first():
        phi[0:reduced, :] = all_s[...]

    def products(i, row):
        phi[row : row + reduced - i, :] = all_s[i : i + 1, :] * all_s[i:reduced, :]

    def ending(row):
        phi[row : row + 1, :] = all_u[...]
        phi[row + 1 : row + 2, :] = jnp.ones((1, count), F32)
        if row + 2 < phi.shape[0]:
            phi[row + 2 :, :] = jnp.zeros((phi.shape[0] - row - 2, count), F32)

    steps = [first]
    row = reduced
    for i in range(reduced):
        steps.append(functools.partial(products, i, row))
        row += reduced - i
    steps.append(functools.partial(ending, row))

    def narrow(rows):
        high_p[rows, :], low_p[rows, :] = split(phi[rows, :])

    for k in range(0, phi.shape[0], LANES):
        steps.append(functools.partial(narrow, slice(k, k + LANES)))
    return steps


def lanes_of(value):
    return jnp.sum(value.reshape(-1, value.shape[-1]), axis=0, keepdims=True)


def second_kernel(
    all_s, all_u, all_t, high_a, low_a, begin, inverse, info, after, duals, last, history,
    phi, high_p, low_p, high_w, low_w, better, high_b, low_b, gap, answer,
    own1, own2, land1, land2, out1, out2, mean1, mean2, mine, ship, span,
    send1, recv1, spread1, got1, send2, recv2, spread2, got2, ship_send, ship_recv,
    *, width, first_owners, second_owners, order,
):
    slabs = lax.axis_size("slab")
    feats = lax.axis_size("feat")
    me = lax.axis_index("slab")
    core = lax.axis_index("feat")
    owners, reduced, wide = own1.shape
    half = reduced // feats
    count = all_s.shape[1]
    head = feats - 1
    leading = core == head
    everyones = sorted(set(first_owners) | set(second_owners))

    def among(slab_list):
        return functools.reduce(jnp.logical_or, [me == slab for slab in slab_list])

    def place_in(slab_list):
        return functools.reduce(lambda a, b: a + b, [jnp.where(me == slab, k, 0) for k, slab in enumerate(slab_list)])

    inside, inside1, inside2 = among(everyones), among(first_owners), among(second_owners)
    spot1, spot2 = place_in(first_owners), place_in(second_owners)

    def copy(source, target, send, recv, slab, feat):
        return pltpu.make_async_remote_copy(
            src_ref=source, dst_ref=target, send_sem=send, recv_sem=recv,
            device_id={"slab": slab, "feat": feat}, device_id_type=pl.DeviceIdType.MESH,
        )

    def arrived(target, size, sem):
        part = target.at[pl.ds(0, size)]
        copy(part, part, sem, sem, me, core).wait_recv()

    def departed(source, size, sem):
        part = source.at[pl.ds(0, size)]
        copy(part, part, sem, sem, me, core).wait_send()

    def each(order, body):
        if len(order) <= 16:
            for d in order:
                body(d)
            return

        def step(d, carry):
            body(d)
            return carry

        lax.fori_loop(min(order), max(order) + 1, step, 0)

    far = sorted(range(1, slabs), key=lambda d: -min(d, slabs - d))

    def slab_of(d):
        return lax.rem(me + d, slabs)

    def split_on(flag, yes, no):
        pl.when(flag)(yes)
        pl.when(jnp.logical_not(flag))(no)

    barrier = pltpu.get_barrier_semaphore()

    def greet(slab, feat):
        pl.semaphore_signal(
            barrier, inc=1, device_id={"slab": slab, "feat": feat}, device_id_type=pl.DeviceIdType.MESH
        )

    @pl.when(leading & inside)
    def _():
        for f in range(feats):
            each(far, lambda d, f=f: greet(slab_of(d), f))
        for f in range(head):
            greet(me, f)

    @pl.when(jnp.logical_not(leading & inside))
    def _():
        for slab in everyones:
            greet(slab, head)

    @pl.when(leading & jnp.logical_not(inside))
    def _():
        for f in range(head):
            greet(me, f)

    @pl.when(jnp.logical_not(leading) & jnp.logical_not(inside))
    def _():
        greet(me, head)

    def scatter(source, landing, send, recv, slab_list, group):
        for k, slab in enumerate(slab_list):
            if k not in group:
                continue

            @pl.when(me != slab)
            def _():
                copy(source.at[k], landing.at[me], send, recv, slab, head).start()

    def joined(buffer, rows):
        return jnp.concatenate([buffer[k][:rows] for k in range(owners)], 1)

    def owner_first():
        land1[me] = own1[spot1]
        arrived(land1, slabs - 1, recv1)
        out1[...] = land1[...].sum(0) * (1.0 / slabs)
        each(far, lambda d: copy(out1, mean1.at[spot1], spread1, got1, slab_of(d), head).start())
        mean1[spot1] = out1[...]

    def owner_second():
        old = mean1[spot2]
        dual1 = lanes_of(jnp.square(old))
        land2[me] = own2[spot2]
        arrived(land2, slabs - 1, recv2)
        whole = land2[...].sum(0)
        new = whole[:reduced] * (1.0 / slabs)
        primal2 = lanes_of(jnp.square(land2[:, 0:reduced] - new[None]))
        dual2 = lanes_of(jnp.square(new - old))
        scale = slabs * penalty * penalty
        stats = jnp.concatenate([whole[reduced : reduced + 1], primal2, dual1 * scale, dual2 * scale], 0)
        for f in range(feats):
            out2[f, 0:half] = new[f * half : (f + 1) * half]
            out2[f, half : half + 4] = stats

        def one(slab):
            for f in range(feats):

                @pl.when((me != slab) | (f != head))
                def _():
                    copy(out2.at[f], mean2.at[spot2], spread2, got2, slab, f).start()

        for slab in order:
            one(slab)
        mean2[spot2] = out2[head]

    near_half = -(-owners // 2)
    groups = (range(0, near_half), range(near_half, owners))

    def leader():
        ah, al = high_a[...], low_a[...]
        delta = info[0:1, 0:1]
        kept = info[0:1, 1:2] > 0.5
        middle = up(count // 2, LANES)
        parts = (slice(0, middle), slice(middle, count))
        steps = feature_steps(all_s, all_u, phi, high_p, low_p)
        chunk = -(-len(steps) // (2 * STEPS))
        old, fresh, spare = begin, high_b, low_b
        size = jnp.ones((1, 1), F32)
        for step in range(STEPS):
            c, delta = newton_scale(delta)
            for part in parts:
                gap[:, part] = dot(ah, old[:, part]).astype(BF16)
                for _ in range(min(chunk, len(steps))):
                    steps.pop(0)()
            x = old[...]
            for part in parts:
                value = (2.0 / size) * old[:, part].astype(F32) - dot(x, gap[:, part])
                if step == STEPS - 1:
                    value = value * (c * size * size)
                fresh[:, part] = value.astype(BF16)
            size = c * size * size
            old, fresh, spare = fresh, spare, fresh
        b = all_t[...] * (1.0 / count)
        x = old[...]
        for part in parts:
            less_eye(dot(ah, x[:, part]) + dot(al, x[:, part]), gap, part)
        c, _ = newton_scale(delta)
        for part in parts:
            value = c * (x[:, part].astype(F32) - dot(x, gap[:, part]))
            better[:, part] = jnp.where(kept, inverse[:, part], value)
        high_b[...], low_b[...] = split(better[...])
        xh, xl = high_b[...], low_b[...]
        y = thin(b, xh, xl)
        y = y + thin(b - thin(y, ah, al), xh, xl)
        y = y + thin(b - thin(y, ah, al), xh, xl)
        answer[...] = y
        for group in groups:
            across = slice(group.start * wide, group.stop * wide)
            start_value = thin(y, high_p[across, :], low_p[across, :], NT)
            for k in group:
                near = (k - group.start) * wide
                own1[k] = start_value[:, near : near + wide]
            if group is groups[0]:
                split_on(
                    inside,
                    lambda: pl.semaphore_wait(barrier, slabs * feats - 1),
                    lambda: pl.semaphore_wait(barrier, len(everyones) + feats - 1),
                )
            scatter(own1, land1, send1, recv1, first_owners, group)

        for _ in range(2):
            bh, bl = high_b[...], low_b[...]
            for part in parts:
                less_eye(dot(ah, bh[:, part]) + (dot(ah, bl[:, part]) + dot(al, bh[:, part])), gap, part)
            for part in parts:
                better[:, part] = better[:, part] - dot(bh, gap[:, part])
            high_b[...], low_b[...] = split(better[...])
        pl.when(inside1)(owner_first)
        weights = dot(high_b[...], high_p[...], NT) + (
            dot(high_b[...], low_p[...], NT) + dot(low_b[...], high_p[...], NT)
        )
        high_w[...], low_w[...] = split(weights)

        split_on(
            inside1,
            lambda: arrived(mean1, owners - 1, got1),
            lambda: arrived(mean1, owners, got1),
        )
        first = joined(own1, reduced)
        mean = joined(mean1, reduced)
        v = thin(mean, high_p[...], low_p[...]) * (2.0 / (count * penalty)) + answer[...]
        primal1 = jnp.sum(jnp.square(first - mean), axis=0, keepdims=True)
        results = []
        for group in groups:
            across = slice(group.start * wide, group.stop * wide)
            result = first[:, across] + 2.0 * mean[:, across] - thin(v, high_w[:, across], low_w[:, across])
            for k in group:
                near = (k - group.start) * wide
                own2[k, 0:reduced] = result[:, near : near + wide]
                own2[k, reduced : reduced + 1] = primal1[:, k * wide : (k + 1) * wide]
            scatter(own2, land2, send2, recv2, second_owners, group)
            results.append(result)
        result = jnp.concatenate(results, 1)
        change = (first - mean) + result
        for f in range(head):
            ship[f, 0] = result[f * half : (f + 1) * half]
            ship[f, 1] = change[f * half : (f + 1) * half]
            copy(ship.at[f], mine, ship_send.at[f], ship_recv, me, f).start()
        mine[0] = result[head * half :]
        mine[1] = change[head * half :]
        pl.when(inside2)(owner_second)

        split_on(inside1, lambda: departed(own1, owners - 1, send1), lambda: departed(own1, owners, send1))
        split_on(inside2, lambda: departed(own2, owners - 1, send2), lambda: departed(own2, owners, send2))
        for f in range(head):
            copy(ship.at[f], mine, ship_send.at[f], ship_recv, me, core).wait_send()

    def follower():
        split_on(
            inside,
            lambda: pl.semaphore_wait(barrier, len(everyones)),
            lambda: pl.semaphore_wait(barrier, len(everyones) + 1),
        )
        copy(ship.at[0], mine, ship_send.at[0], ship_recv, me, core).wait_recv()

    split_on(leading, leader, follower)
    split_on(
        leading & inside2,
        lambda: arrived(mean2, owners - 1, got2),
        lambda: arrived(mean2, owners, got2),
    )
    new = joined(mean2, half)
    after[...] = mine[0]
    last[...] = new
    duals[...] = mine[1] - new
    sums = mean2[0][half : half + 4]
    for k in range(1, owners):
        sums = sums + mean2[k][half : half + 4]
    sums = jnp.sum(sums, axis=1, keepdims=True)
    history[...] = jnp.broadcast_to(jnp.sqrt(sums * (1.0 / (slabs * reduced * width))), history.shape)

    @pl.when(leading & inside1)
    def _():
        departed(land1, slabs - 1, spread1)

    @pl.when(leading & inside2)
    def _():
        departed(span, slabs * feats - 1, spread2)


def last_kernel(after, duals, last, history, out_after, out_duals, out_last, out_history):
    half, width = out_last.shape
    for r in range(half):
        out_after[r] = after[r : r + 1, :width]
        out_duals[r] = duals[r : r + 1, :width]
    out_last[...] = last[:, :width]
    for r in range(2):
        out_history[r : r + 1, :] = jnp.concatenate([history[2 * r + k : 2 * r + k + 1, 0:1] for k in range(2)], 1)


def shards(states, inputs, targets, *, spots):
    reduced, own = states.shape
    feats = lax.axis_size("feat")
    slabs = lax.axis_size("slab")
    half = reduced // feats
    width = reduced + reduced * (reduced + 1) // 2 + 2
    count = own * feats
    tiles = up(width, LANES) // LANES
    wide = -(-tiles // slabs) * LANES
    columns = up(width, wide)
    owners = columns // wide
    vmem = pl.BlockSpec(memory_space=pltpu.VMEM)
    dma = pltpu.SemaphoreType.DMA

    def shape(*sizes, dtype=F32):
        return jax.ShapeDtypeStruct(sizes, dtype)

    def hold(*sizes, dtype=F32):
        return pltpu.VMEM(sizes, dtype)

    gathered = pl.pallas_call(
        exchange_kernel,
        out_shape=(shape(reduced, count), shape(1, count), shape(reduced, count)),
        in_specs=[pl.BlockSpec(memory_space=pltpu.HBM)] * 3,
        out_specs=(vmem,) * 3,
        scratch_shapes=[dma((3,)), dma((3,)), dma((feats, 3))],
        compiler_params=pltpu.CompilerParams(vmem_limit_bytes=LIMIT, collective_id=1, has_side_effects=True),
        name="exchange",
    )(*[pltpu.with_memory_space_constraint(x, pltpu.HBM) for x in (states, inputs[None], targets)])
    square = shape(count, count)
    short = shape(count, count, dtype=BF16)
    solved = pl.pallas_call(
        inverse_kernel,
        out_shape=(short, short, short, square, shape(1, LANES)),
        in_specs=[vmem] * 2,
        out_specs=(vmem,) * 5,
        scratch_shapes=[
            hold(count, count), hold(count, count, dtype=BF16),
            hold(count, count, dtype=BF16), hold(count, count, dtype=BF16),
        ],
        compiler_params=pltpu.CompilerParams(vmem_limit_bytes=LIMIT),
        name="local_inverse",
    )(gathered[0], gathered[1])
    block = shape(half, columns)
    first_owners, second_owners, order = choose(spots, owners)
    after, duals, last, history = pl.pallas_call(
        functools.partial(
            second_kernel, width=width, first_owners=first_owners, second_owners=second_owners, order=order
        ),
        out_shape=(block, block, block, shape(4, LANES)),
        in_specs=[vmem] * 8,
        out_specs=(vmem,) * 4,
        scratch_shapes=[
            hold(columns, count),
            hold(columns, count, dtype=BF16), hold(columns, count, dtype=BF16),
            hold(count, columns, dtype=BF16), hold(count, columns, dtype=BF16),
            hold(count, count), hold(count, count, dtype=BF16), hold(count, count, dtype=BF16),
            hold(count, count, dtype=BF16), hold(reduced, count),
            hold(owners, reduced, wide), hold(owners, reduced + 1, wide),
            hold(slabs, reduced, wide), hold(slabs, reduced + 1, wide),
            hold(reduced, wide), hold(feats, half + 4, wide),
            hold(owners, reduced, wide), hold(owners, half + 4, wide),
            hold(2, half, columns), hold(max(feats - 1, 1), 2, half, columns),
            hold(slabs * feats, half + 4, wide),
            dma, dma, dma, dma, dma, dma, dma, dma, dma((max(feats - 1, 1),)), dma,
        ],
        compiler_params=pltpu.CompilerParams(vmem_limit_bytes=2 * LIMIT, collective_id=0, has_side_effects=True),
        name="second_and_averages",
    )(*gathered, *solved)
    shard = shape(half, width)
    spread_rows = shape(half, 1, width)
    after, duals, last, history = pl.pallas_call(
        last_kernel,
        out_shape=(spread_rows, spread_rows, shard, shape(2, 2)),
        in_specs=[vmem] * 4,
        out_specs=(vmem,) * 4,
        compiler_params=pltpu.CompilerParams(vmem_limit_bytes=4 * 2**20),
        name="outputs",
    )(after, duals, last, history)
    return (jnp.swapaxes(after, 0, 1), jnp.swapaxes(duals, 0, 1), last, history)


def choose(spots, owners):
    slabs = range(len(spots))
    apart = [[sum(abs(a - b) for a, b in zip(spots[p], spots[q])) for q in slabs] for p in slabs]
    first = sorted(slabs, key=lambda q: (max(apart[q]), -apart[0][q], q))[:owners]
    second = sorted(slabs, key=lambda q: (max(apart[q]), apart[0][q], q))[:owners]
    return sorted(first), sorted(second), sorted(slabs, key=lambda p: (apart[0][p], p))


def solution(mesh):
    spots = [
        tuple(getattr(device, "coords", None) or (index,)) for index, device in enumerate(mesh.devices[:, 0])
    ]
    in_specs = (P(None, ("slab", "feat")), P(("slab", "feat")), P(None, ("slab", "feat")))
    out_specs = (P("slab", "feat", None), P("slab", "feat", None), P("feat", None), P())
    body = functools.partial(shards, spots=spots)
    return jax.shard_map(body, mesh=mesh, in_specs=in_specs, out_specs=out_specs, check_vma=False)
```

```python
import functools

import jax
import jax.numpy as jnp
from jax import lax
from jax.experimental import pallas as pl
from jax.experimental.pallas import tpu as pltpu
from jax.sharding import PartitionSpec as P

penalty = 1.0
LIMIT = 20 * 2**20
LANES = 128
STEPS = 3
EASY = 200.0
NN = (((1,), (0,)), ((), ()))
NT = (((1,), (1,)), ((), ()))
TN = (((0,), (0,)), ((), ()))
F32 = jnp.float32
BF16 = jnp.bfloat16


def up(value, step):
    return -(-value // step) * step


def dot(left, right, dims=NN):
    return lax.dot_general(left.astype(BF16), right.astype(BF16), dims, preferred_element_type=F32)


def split(value):
    high = value.astype(BF16)
    return high, (value - high.astype(F32)).astype(BF16)


def thin(left, high, low, dims=NN):
    rows = left.shape[0]
    top = left.astype(BF16).astype(F32)
    both = jnp.concatenate([top, left - top], 0).astype(BF16)
    out = dot(both, high, dims) + dot(both, low, dims)
    return out[:rows] + out[rows:]


def eye_mask(size):
    return lax.broadcasted_iota(jnp.int32, (size, size), 0) == lax.broadcasted_iota(jnp.int32, (size, size), 1)


def eye(size):
    return jnp.where(eye_mask(size), 1.0, 0.0)


def less_eye(value, target, part):
    for p in range(0, value.shape[0], LANES):
        for q in range(part.start, part.stop, LANES):
            piece = value[p : p + LANES, q - part.start : q - part.start + LANES]
            piece = piece - eye(LANES) if p == q else piece
            target[p : p + LANES, q : q + LANES] = piece.astype(BF16)


def invert_by_pivots(source, target):
    size = source.shape[0]
    target[...] = source[...]
    sub = lax.broadcasted_iota(jnp.int32, (size, 1), 0)
    lane = lax.broadcasted_iota(jnp.int32, (1, size), 1)

    def step(k, carry):
        row = target[pl.ds(k, 1), :]
        here = lane == k
        pivot = jnp.sum(jnp.where(here, row, 0.0), axis=1, keepdims=True)
        scaled = jnp.where(here, 1.0, row) / pivot
        whole = target[...]
        column = jnp.sum(jnp.where(here, whole, 0.0), axis=1, keepdims=True)
        column = jnp.where(sub == k, -1.0, column)
        kept = jnp.where(here | (sub == k), 0.0, whole)
        target[...] = kept - column * scaled
        return carry

    lax.fori_loop(0, size, step, 0)


def exchange_kernel(states, inputs, targets, all_s, all_u, all_t, local, send, recv):
    feats = lax.axis_size("feat")
    core = lax.axis_index("feat")
    head = feats - 1
    own = states.shape[1]
    sources = (states, inputs, targets)
    alls = (all_s, all_u, all_t)

    def load(i):
        return pltpu.make_async_copy(sources[i], alls[i].at[:, pl.ds(head * own, own)], local.at[i])

    def move(i, f):
        return pltpu.make_async_remote_copy(
            src_ref=sources[i], dst_ref=alls[i].at[:, pl.ds(f * own, own)],
            send_sem=send.at[i], recv_sem=recv.at[f, i],
            device_id={"feat": head}, device_id_type=pl.DeviceIdType.MESH,
        )

    barrier = pltpu.get_barrier_semaphore()

    def greet(feat):
        pl.semaphore_signal(barrier, inc=1, device_id={"feat": feat}, device_id_type=pl.DeviceIdType.MESH)

    @pl.when(core == head)
    def _():
        for f in range(head):
            greet(f)
        for i in range(3):
            load(i).start()
        pl.semaphore_wait(barrier, head)
        for i in range(3):
            load(i).wait()
        for f in range(head):
            for i in range(3):
                move(i, f).wait_recv()

    for f in range(head):

        @pl.when(core == f)
        def _():
            greet(head)
            pl.semaphore_wait(barrier, 1)
            for i in range(3):
                move(i, f).start()
            for i in range(3):
                move(i, f).wait_send()


def stacked(value, orders):
    parts = []
    rest = value
    for _ in range(1 + max(max(order) for order in orders)):
        high = rest.astype(BF16).astype(F32)
        parts.append(high)
        rest = rest - high
    left = jnp.concatenate([parts[i] for i, _ in orders], 0)
    right = jnp.concatenate([parts[j] for _, j in orders], 0)
    return left.astype(BF16), right.astype(BF16)


def newton_scale(delta):
    return 2.0 / (2.0 - delta * delta), delta * delta / (2.0 - delta * delta)


def inverse_kernel(all_s, all_u, high_a, low_a, start, inverse, info, system, shifted, high_x, low_x):
    reduced, count = all_s.shape
    edge = LANES
    spans = [slice(k, k + edge) for k in range(0, count, edge)]

    def solve():
        s = all_s[...]
        sub = lax.broadcasted_iota(jnp.int32, (8, count), 0)
        last = jnp.where(sub == 0, all_u[...], jnp.where(sub == 1, 1.0, 0.0)) * (1.0 / count) ** 0.5
        left, right = stacked(s * (0.5 / count) ** 0.25, ((0, 0), (0, 1), (1, 0), (0, 2), (2, 0), (1, 1)))
        extra = jnp.concatenate([s * s * (0.5 / count) ** 0.5, last], 0)
        left2, right2 = stacked(extra, ((0, 0), (0, 1), (1, 0)))
        sums = [jnp.zeros((8, edge), F32)] * len(spans)
        for p, down in enumerate(spans):
            inner = dot(left[:, down], right, TN)
            other = dot(left2[:, down], right2, TN)
            for q, across in enumerate(spans):
                part = inner[:, across]
                part = part * (part + (2.0 / count) ** 0.5) + other[:, across]
                if p == q:
                    part = part + jnp.where(eye_mask(edge), penalty, 0.0)
                system[down, across] = part
                high_a[down, across], low_a[down, across] = split(part)
                size = jnp.abs(part)
                shifted[down, across] = size.astype(BF16)
                sums[q] = sums[q] + size.reshape(edge // 8, 8, edge).sum(0)
        sums = jnp.concatenate([jnp.broadcast_to(jnp.sum(part, axis=0, keepdims=True), (8, edge)) for part in sums], 1)
        trial = sums.astype(BF16)
        high = jnp.max(dot(trial, shifted[...]) / trial.astype(F32)) * (1.005 / penalty)
        delta = (high - 1.0) / (high + 1.0)
        alpha = 2.0 / ((1.0 + high) * penalty)
        c, later = newton_scale(delta)

        def begin(target, dtype):
            for p, down in enumerate(spans):
                for q, across in enumerate(spans):
                    part = (-c * alpha * alpha) * system[down, across]
                    if p == q:
                        part = part + jnp.where(eye_mask(edge), 2.0 * c * alpha, 0.0)
                    target[down, across] = part.astype(dtype)

        begin(start, BF16)
        hard = jnp.logical_not(high <= EASY)
        lane = lax.broadcasted_iota(jnp.int32, (1, LANES), 1)
        info[...] = jnp.where(lane == 0, later, jnp.where(hard, 1.0, 0.0))

        @pl.when(hard)
        def _():
            begin(inverse, F32)
            careful(later)

    def careful(delta):
        sub = lax.broadcasted_iota(jnp.int32, (8, count), 0)
        mixed = (lax.broadcasted_iota(jnp.int32, (8, count), 1) + 1) * (sub * 40503 + 30011)
        mixed = (mixed ^ (mixed >> 7)) * 9973
        signs = jnp.where(((mixed >> 9) & 1) == 1, 1.0, -1.0)

        def coarse(state):
            step, delta = state
            x = inverse[...].astype(BF16)
            shifted[...] = dot(high_a[...], x).astype(BF16)
            c, later = newton_scale(delta)
            inverse[...] = c * (2.0 * inverse[...] - dot(x, shifted[...]))
            return step + 1, later

        lax.while_loop(lambda state: (state[1] > 0.085) & (state[0] < 12), coarse, (0, delta))

        def polish(state):
            step, _ = state
            high_x[...], low_x[...] = split(inverse[...])
            ah, al, xh, xl = high_a[...], low_a[...], high_x[...], low_x[...]
            shifted[...] = (eye(count) - (dot(ah, xh) + (dot(ah, xl) + dot(al, xh)))).astype(BF16)
            once = signs - thin(thin(signs, xh, xl), ah, al)
            twice = once - thin(thin(once, xh, xl), ah, al)
            inverse[...] = inverse[...] + dot(xh, shifted[...])
            return step + 1, jnp.sum(twice * twice) * (1.0 / 8.0)

        _, worst = lax.while_loop(
            lambda state: jnp.logical_not(state[1] < 0.001) & (state[0] < 8), polish, (0, jnp.float32(1e9))
        )

        @pl.when(jnp.logical_not(worst < 0.001))
        def _():
            invert_by_pivots(system, inverse)

    pl.when(lax.axis_index("feat") == lax.axis_size("feat") - 1)(solve)


def feature_steps(all_s, all_u, phi, high_p, low_p):
    reduced, count = all_s.shape

    def first():
        phi[0:reduced, :] = all_s[...]

    def products(i, row):
        phi[row : row + reduced - i, :] = all_s[i : i + 1, :] * all_s[i:reduced, :]

    def ending(row):
        phi[row : row + 1, :] = all_u[...]
        phi[row + 1 : row + 2, :] = jnp.ones((1, count), F32)
        if row + 2 < phi.shape[0]:
            phi[row + 2 :, :] = jnp.zeros((phi.shape[0] - row - 2, count), F32)

    steps = [first]
    row = reduced
    for i in range(reduced):
        steps.append(functools.partial(products, i, row))
        row += reduced - i
    steps.append(functools.partial(ending, row))

    def narrow(rows):
        high_p[rows, :], low_p[rows, :] = split(phi[rows, :])

    for k in range(0, phi.shape[0], LANES):
        steps.append(functools.partial(narrow, slice(k, k + LANES)))
    return steps


def lanes_of(value):
    return jnp.sum(value.reshape(-1, value.shape[-1]), axis=0, keepdims=True)


def second_kernel(
    all_s, all_u, all_t, high_a, low_a, begin, inverse, info, after, duals, last, history,
    phi, high_p, low_p, high_w, low_w, better, high_b, low_b, gap, answer,
    own1, own2, land1, land2, out1, out2, mean1, mean2, mine, ship, span,
    send1, recv1, spread1, got1, send2, recv2, spread2, got2, ship_send, ship_recv,
    *, width, first_owners, second_owners, order,
):
    slabs = lax.axis_size("slab")
    feats = lax.axis_size("feat")
    me = lax.axis_index("slab")
    core = lax.axis_index("feat")
    owners, reduced, wide = own1.shape
    half = reduced // feats
    count = all_s.shape[1]
    head = feats - 1
    leading = core == head
    everyones = sorted(set(first_owners) | set(second_owners))

    def among(slab_list):
        return functools.reduce(jnp.logical_or, [me == slab for slab in slab_list])

    def place_in(slab_list):
        return functools.reduce(lambda a, b: a + b, [jnp.where(me == slab, k, 0) for k, slab in enumerate(slab_list)])

    inside, inside1, inside2 = among(everyones), among(first_owners), among(second_owners)
    spot1, spot2 = place_in(first_owners), place_in(second_owners)

    def copy(source, target, send, recv, slab, feat):
        return pltpu.make_async_remote_copy(
            src_ref=source, dst_ref=target, send_sem=send, recv_sem=recv,
            device_id={"slab": slab, "feat": feat}, device_id_type=pl.DeviceIdType.MESH,
        )

    def arrived(target, size, sem):
        part = target.at[pl.ds(0, size)]
        copy(part, part, sem, sem, me, core).wait_recv()

    def departed(source, size, sem):
        part = source.at[pl.ds(0, size)]
        copy(part, part, sem, sem, me, core).wait_send()

    def each(order, body):
        if len(order) <= 16:
            for d in order:
                body(d)
            return

        def step(d, carry):
            body(d)
            return carry

        lax.fori_loop(min(order), max(order) + 1, step, 0)

    far = sorted(range(1, slabs), key=lambda d: -min(d, slabs - d))

    def slab_of(d):
        return lax.rem(me + d, slabs)

    def split_on(flag, yes, no):
        pl.when(flag)(yes)
        pl.when(jnp.logical_not(flag))(no)

    barrier = pltpu.get_barrier_semaphore()

    def greet(slab, feat):
        pl.semaphore_signal(
            barrier, inc=1, device_id={"slab": slab, "feat": feat}, device_id_type=pl.DeviceIdType.MESH
        )

    @pl.when(leading & inside)
    def _():
        for f in range(feats):
            each(far, lambda d, f=f: greet(slab_of(d), f))
        for f in range(head):
            greet(me, f)

    @pl.when(jnp.logical_not(leading & inside))
    def _():
        for slab in everyones:
            greet(slab, head)

    @pl.when(leading & jnp.logical_not(inside))
    def _():
        for f in range(head):
            greet(me, f)

    @pl.when(jnp.logical_not(leading) & jnp.logical_not(inside))
    def _():
        greet(me, head)

    def scatter(source, landing, send, recv, slab_list, group):
        for k, slab in enumerate(slab_list):
            if k not in group:
                continue

            @pl.when(me != slab)
            def _():
                copy(source.at[k], landing.at[me], send, recv, slab, head).start()

    def joined(buffer, rows):
        return jnp.concatenate([buffer[k][:rows] for k in range(owners)], 1)

    def owner_first():
        land1[me] = own1[spot1]
        arrived(land1, slabs - 1, recv1)
        out1[...] = land1[...].sum(0) * (1.0 / slabs)
        each(far, lambda d: copy(out1, mean1.at[spot1], spread1, got1, slab_of(d), head).start())
        mean1[spot1] = out1[...]

    def owner_second():
        old = mean1[spot2]
        dual1 = lanes_of(jnp.square(old))
        land2[me] = own2[spot2]
        arrived(land2, slabs - 1, recv2)
        whole = land2[...].sum(0)
        new = whole[:reduced] * (1.0 / slabs)
        primal2 = lanes_of(jnp.square(land2[:, 0:reduced] - new[None]))
        dual2 = lanes_of(jnp.square(new - old))
        scale = slabs * penalty * penalty
        stats = jnp.concatenate([whole[reduced : reduced + 1], primal2, dual1 * scale, dual2 * scale], 0)
        for f in range(feats):
            out2[f, 0:half] = new[f * half : (f + 1) * half]
            out2[f, half : half + 4] = stats

        def one(slab):
            for f in range(feats):

                @pl.when((me != slab) | (f != head))
                def _():
                    copy(out2.at[f], mean2.at[spot2], spread2, got2, slab, f).start()

        for slab in order:
            one(slab)
        mean2[spot2] = out2[head]

    near_half = -(-owners // 3)
    groups = [range(k, min(k + near_half, owners)) for k in range(0, owners, near_half)]

    def leader():
        ah, al = high_a[...], low_a[...]
        delta = info[0:1, 0:1]
        kept = info[0:1, 1:2] > 0.5
        middle = up(count // 2, LANES)
        parts = (slice(0, middle), slice(middle, count))
        steps = feature_steps(all_s, all_u, phi, high_p, low_p)
        chunk = -(-len(steps) // (2 * STEPS))
        old, fresh, spare = begin, high_b, low_b
        size = jnp.ones((1, 1), F32)
        for step in range(STEPS):
            c, delta = newton_scale(delta)
            for part in parts:
                gap[:, part] = dot(ah, old[:, part]).astype(BF16)
                for _ in range(min(chunk, len(steps))):
                    steps.pop(0)()
            x = old[...]
            for part in parts:
                value = (2.0 / size) * old[:, part].astype(F32) - dot(x, gap[:, part])
                if step == STEPS - 1:
                    value = value * (c * size * size)
                fresh[:, part] = value.astype(BF16)
            size = c * size * size
            old, fresh, spare = fresh, spare, fresh
        b = all_t[...] * (1.0 / count)
        x = old[...]
        for part in parts:
            less_eye(dot(ah, x[:, part]) + dot(al, x[:, part]), gap, part)
        c, _ = newton_scale(delta)
        for part in parts:
            value = c * (x[:, part].astype(F32) - dot(x, gap[:, part]))
            better[:, part] = jnp.where(kept, inverse[:, part], value)
        high_b[...], low_b[...] = split(better[...])
        xh, xl = high_b[...], low_b[...]
        y = thin(b, xh, xl)
        y = y + thin(b - thin(y, ah, al), xh, xl)
        y = y + thin(b - thin(y, ah, al), xh, xl)
        answer[...] = y
        for group in groups:
            across = slice(group.start * wide, group.stop * wide)
            start_value = thin(y, high_p[across, :], low_p[across, :], NT)
            for k in group:
                near = (k - group.start) * wide
                own1[k] = start_value[:, near : near + wide]
            if group is groups[0]:
                split_on(
                    inside,
                    lambda: pl.semaphore_wait(barrier, slabs * feats - 1),
                    lambda: pl.semaphore_wait(barrier, len(everyones) + feats - 1),
                )
            scatter(own1, land1, send1, recv1, first_owners, group)

        for _ in range(2):
            bh, bl = high_b[...], low_b[...]
            for part in parts:
                less_eye(dot(ah, bh[:, part]) + (dot(ah, bl[:, part]) + dot(al, bh[:, part])), gap, part)
            for part in parts:
                better[:, part] = better[:, part] - dot(bh, gap[:, part])
            high_b[...], low_b[...] = split(better[...])
        pl.when(inside1)(owner_first)
        weights = dot(high_b[...], high_p[...], NT) + (
            dot(high_b[...], low_p[...], NT) + dot(low_b[...], high_p[...], NT)
        )
        high_w[...], low_w[...] = split(weights)

        split_on(
            inside1,
            lambda: arrived(mean1, owners - 1, got1),
            lambda: arrived(mean1, owners, got1),
        )
        first = joined(own1, reduced)
        mean = joined(mean1, reduced)
        v = thin(mean, high_p[...], low_p[...]) * (2.0 / (count * penalty)) + answer[...]
        primal1 = jnp.sum(jnp.square(first - mean), axis=0, keepdims=True)
        results = []
        for group in groups:
            across = slice(group.start * wide, group.stop * wide)
            result = first[:, across] + 2.0 * mean[:, across] - thin(v, high_w[:, across], low_w[:, across])
            for k in group:
                near = (k - group.start) * wide
                own2[k, 0:reduced] = result[:, near : near + wide]
                own2[k, reduced : reduced + 1] = primal1[:, k * wide : (k + 1) * wide]
            scatter(own2, land2, send2, recv2, second_owners, group)
            results.append(result)
        result = jnp.concatenate(results, 1)
        change = (first - mean) + result
        for f in range(head):
            ship[f, 0] = result[f * half : (f + 1) * half]
            ship[f, 1] = change[f * half : (f + 1) * half]
            copy(ship.at[f], mine, ship_send.at[f], ship_recv, me, f).start()
        mine[0] = result[head * half :]
        mine[1] = change[head * half :]
        pl.when(inside2)(owner_second)

        split_on(inside1, lambda: departed(own1, owners - 1, send1), lambda: departed(own1, owners, send1))
        split_on(inside2, lambda: departed(own2, owners - 1, send2), lambda: departed(own2, owners, send2))
        for f in range(head):
            copy(ship.at[f], mine, ship_send.at[f], ship_recv, me, core).wait_send()

    def follower():
        split_on(
            inside,
            lambda: pl.semaphore_wait(barrier, len(everyones)),
            lambda: pl.semaphore_wait(barrier, len(everyones) + 1),
        )
        copy(ship.at[0], mine, ship_send.at[0], ship_recv, me, core).wait_recv()

    split_on(leading, leader, follower)
    split_on(
        leading & inside2,
        lambda: arrived(mean2, owners - 1, got2),
        lambda: arrived(mean2, owners, got2),
    )
    new = joined(mean2, half)
    after[...] = mine[0]
    last[...] = new
    duals[...] = mine[1] - new
    sums = mean2[0][half : half + 4]
    for k in range(1, owners):
        sums = sums + mean2[k][half : half + 4]
    sums = jnp.sum(sums, axis=1, keepdims=True)
    history[...] = jnp.broadcast_to(jnp.sqrt(sums * (1.0 / (slabs * reduced * width))), history.shape)

    @pl.when(leading & inside1)
    def _():
        departed(land1, slabs - 1, spread1)

    @pl.when(leading & inside2)
    def _():
        departed(span, slabs * feats - 1, spread2)


def last_kernel(after, duals, last, history, out_after, out_duals, out_last, out_history):
    half, width = out_last.shape
    for r in range(half):
        out_after[r] = after[r : r + 1, :width]
        out_duals[r] = duals[r : r + 1, :width]
    out_last[...] = last[:, :width]
    for r in range(2):
        out_history[r : r + 1, :] = jnp.concatenate([history[2 * r + k : 2 * r + k + 1, 0:1] for k in range(2)], 1)


def shards(states, inputs, targets, *, spots):
    reduced, own = states.shape
    feats = lax.axis_size("feat")
    slabs = lax.axis_size("slab")
    half = reduced // feats
    width = reduced + reduced * (reduced + 1) // 2 + 2
    count = own * feats
    tiles = up(width, LANES) // LANES
    wide = -(-tiles // slabs) * LANES
    columns = up(width, wide)
    owners = columns // wide
    vmem = pl.BlockSpec(memory_space=pltpu.VMEM)
    dma = pltpu.SemaphoreType.DMA

    def shape(*sizes, dtype=F32):
        return jax.ShapeDtypeStruct(sizes, dtype)

    def hold(*sizes, dtype=F32):
        return pltpu.VMEM(sizes, dtype)

    gathered = pl.pallas_call(
        exchange_kernel,
        out_shape=(shape(reduced, count), shape(1, count), shape(reduced, count)),
        in_specs=[pl.BlockSpec(memory_space=pltpu.HBM)] * 3,
        out_specs=(vmem,) * 3,
        scratch_shapes=[dma((3,)), dma((3,)), dma((feats, 3))],
        compiler_params=pltpu.CompilerParams(vmem_limit_bytes=LIMIT, collective_id=1, has_side_effects=True),
        name="exchange",
    )(*[pltpu.with_memory_space_constraint(x, pltpu.HBM) for x in (states, inputs[None], targets)])
    square = shape(count, count)
    short = shape(count, count, dtype=BF16)
    solved = pl.pallas_call(
        inverse_kernel,
        out_shape=(short, short, short, square, shape(1, LANES)),
        in_specs=[vmem] * 2,
        out_specs=(vmem,) * 5,
        scratch_shapes=[
            hold(count, count), hold(count, count, dtype=BF16),
            hold(count, count, dtype=BF16), hold(count, count, dtype=BF16),
        ],
        compiler_params=pltpu.CompilerParams(vmem_limit_bytes=LIMIT),
        name="local_inverse",
    )(gathered[0], gathered[1])
    block = shape(half, columns)
    first_owners, second_owners, order = choose(spots, owners)
    after, duals, last, history = pl.pallas_call(
        functools.partial(
            second_kernel, width=width, first_owners=first_owners, second_owners=second_owners, order=order
        ),
        out_shape=(block, block, block, shape(4, LANES)),
        in_specs=[vmem] * 8,
        out_specs=(vmem,) * 4,
        scratch_shapes=[
            hold(columns, count),
            hold(columns, count, dtype=BF16), hold(columns, count, dtype=BF16),
            hold(count, columns, dtype=BF16), hold(count, columns, dtype=BF16),
            hold(count, count), hold(count, count, dtype=BF16), hold(count, count, dtype=BF16),
            hold(count, count, dtype=BF16), hold(reduced, count),
            hold(owners, reduced, wide), hold(owners, reduced + 1, wide),
            hold(slabs, reduced, wide), hold(slabs, reduced + 1, wide),
            hold(reduced, wide), hold(feats, half + 4, wide),
            hold(owners, reduced, wide), hold(owners, half + 4, wide),
            hold(2, half, columns), hold(max(feats - 1, 1), 2, half, columns),
            hold(slabs * feats, half + 4, wide),
            dma, dma, dma, dma, dma, dma, dma, dma, dma((max(feats - 1, 1),)), dma,
        ],
        compiler_params=pltpu.CompilerParams(vmem_limit_bytes=2 * LIMIT, collective_id=0, has_side_effects=True),
        name="second_and_averages",
    )(*gathered, *solved)
    shard = shape(half, width)
    spread_rows = shape(half, 1, width)
    after, duals, last, history = pl.pallas_call(
        last_kernel,
        out_shape=(spread_rows, spread_rows, shard, shape(2, 2)),
        in_specs=[vmem] * 4,
        out_specs=(vmem,) * 4,
        compiler_params=pltpu.CompilerParams(vmem_limit_bytes=4 * 2**20),
        name="outputs",
    )(after, duals, last, history)
    return (jnp.swapaxes(after, 0, 1), jnp.swapaxes(duals, 0, 1), last, history)


def choose(spots, owners):
    slabs = range(len(spots))
    apart = [[sum(abs(a - b) for a, b in zip(spots[p], spots[q])) for q in slabs] for p in slabs]
    first = sorted(slabs, key=lambda q: (max(apart[q]), -apart[0][q], q))[:owners]
    second = sorted(slabs, key=lambda q: (max(apart[q]), apart[0][q], q))[:owners]
    return sorted(first), sorted(second), sorted(slabs, key=lambda p: (apart[0][p], p))


def solution(mesh):
    spots = [
        tuple(getattr(device, "coords", None) or (index,)) for index, device in enumerate(mesh.devices[:, 0])
    ]
    in_specs = (P(None, ("slab", "feat")), P(("slab", "feat")), P(None, ("slab", "feat")))
    out_specs = (P("slab", "feat", None), P("slab", "feat", None), P("feat", None), P())
    body = functools.partial(shards, spots=spots)
    return jax.shard_map(body, mesh=mesh, in_specs=in_specs, out_specs=out_specs, check_vma=False)
```

```python
import functools

import jax
import jax.numpy as jnp
from jax import lax
from jax.experimental import pallas as pl
from jax.experimental.pallas import tpu as pltpu
from jax.sharding import PartitionSpec as P

penalty = 1.0
LIMIT = 20 * 2**20
LANES = 128
STEPS = 3
EASY = 200.0
NN = (((1,), (0,)), ((), ()))
NT = (((1,), (1,)), ((), ()))
TN = (((0,), (0,)), ((), ()))
F32 = jnp.float32
BF16 = jnp.bfloat16


def up(value, step):
    return -(-value // step) * step


def dot(left, right, dims=NN):
    return lax.dot_general(left.astype(BF16), right.astype(BF16), dims, preferred_element_type=F32)


def split(value):
    high = value.astype(BF16)
    return high, (value - high.astype(F32)).astype(BF16)


def thin(left, high, low, dims=NN):
    rows = left.shape[0]
    top = left.astype(BF16).astype(F32)
    both = jnp.concatenate([top, left - top], 0).astype(BF16)
    out = dot(both, high, dims) + dot(both, low, dims)
    return out[:rows] + out[rows:]


def eye_mask(size):
    return lax.broadcasted_iota(jnp.int32, (size, size), 0) == lax.broadcasted_iota(jnp.int32, (size, size), 1)


def eye(size):
    return jnp.where(eye_mask(size), 1.0, 0.0)


def less_eye(value, target, part):
    for p in range(0, value.shape[0], LANES):
        for q in range(part.start, part.stop, LANES):
            piece = value[p : p + LANES, q - part.start : q - part.start + LANES]
            piece = piece - eye(LANES) if p == q else piece
            target[p : p + LANES, q : q + LANES] = piece.astype(BF16)


def invert_by_pivots(source, target):
    size = source.shape[0]
    target[...] = source[...]
    sub = lax.broadcasted_iota(jnp.int32, (size, 1), 0)
    lane = lax.broadcasted_iota(jnp.int32, (1, size), 1)

    def step(k, carry):
        row = target[pl.ds(k, 1), :]
        here = lane == k
        pivot = jnp.sum(jnp.where(here, row, 0.0), axis=1, keepdims=True)
        scaled = jnp.where(here, 1.0, row) / pivot
        whole = target[...]
        column = jnp.sum(jnp.where(here, whole, 0.0), axis=1, keepdims=True)
        column = jnp.where(sub == k, -1.0, column)
        kept = jnp.where(here | (sub == k), 0.0, whole)
        target[...] = kept - column * scaled
        return carry

    lax.fori_loop(0, size, step, 0)


def exchange_kernel(states, inputs, targets, all_s, all_u, all_t, local, send, recv):
    feats = lax.axis_size("feat")
    core = lax.axis_index("feat")
    head = feats - 1
    own = states.shape[1]
    sources = (states, inputs, targets)
    alls = (all_s, all_u, all_t)

    def load(i):
        return pltpu.make_async_copy(sources[i], alls[i].at[:, pl.ds(head * own, own)], local.at[i])

    def move(i, f):
        return pltpu.make_async_remote_copy(
            src_ref=sources[i], dst_ref=alls[i].at[:, pl.ds(f * own, own)],
            send_sem=send.at[i], recv_sem=recv.at[f, i],
            device_id={"feat": head}, device_id_type=pl.DeviceIdType.MESH,
        )

    barrier = pltpu.get_barrier_semaphore()

    def greet(feat):
        pl.semaphore_signal(barrier, inc=1, device_id={"feat": feat}, device_id_type=pl.DeviceIdType.MESH)

    @pl.when(core == head)
    def _():
        for f in range(head):
            greet(f)
        for i in range(3):
            load(i).start()
        pl.semaphore_wait(barrier, head)
        for i in range(3):
            load(i).wait()
        for f in range(head):
            for i in range(3):
                move(i, f).wait_recv()

    for f in range(head):

        @pl.when(core == f)
        def _():
            greet(head)
            pl.semaphore_wait(barrier, 1)
            for i in range(3):
                move(i, f).start()
            for i in range(3):
                move(i, f).wait_send()


def stacked(value, orders):
    parts = []
    rest = value
    for _ in range(1 + max(max(order) for order in orders)):
        high = rest.astype(BF16).astype(F32)
        parts.append(high)
        rest = rest - high
    left = jnp.concatenate([parts[i] for i, _ in orders], 0)
    right = jnp.concatenate([parts[j] for _, j in orders], 0)
    return left.astype(BF16), right.astype(BF16)


def newton_scale(delta):
    return 2.0 / (2.0 - delta * delta), delta * delta / (2.0 - delta * delta)


def inverse_kernel(all_s, all_u, high_a, low_a, start, inverse, info, system, shifted, high_x, low_x):
    reduced, count = all_s.shape
    edge = LANES
    spans = [slice(k, k + edge) for k in range(0, count, edge)]

    def solve():
        s = all_s[...]
        sub = lax.broadcasted_iota(jnp.int32, (8, count), 0)
        last = jnp.where(sub == 0, all_u[...], jnp.where(sub == 1, 1.0, 0.0)) * (1.0 / count) ** 0.5
        left, right = stacked(s * (0.5 / count) ** 0.25, ((0, 0), (0, 1), (1, 0), (0, 2), (2, 0), (1, 1)))
        extra = jnp.concatenate([s * s * (0.5 / count) ** 0.5, last], 0)
        left2, right2 = stacked(extra, ((0, 0), (0, 1), (1, 0)))
        sums = [jnp.zeros((8, edge), F32)] * len(spans)
        for p, down in enumerate(spans):
            inner = dot(left[:, down], right, TN)
            other = dot(left2[:, down], right2, TN)
            for q, across in enumerate(spans):
                part = inner[:, across]
                part = part * (part + (2.0 / count) ** 0.5) + other[:, across]
                if p == q:
                    part = part + jnp.where(eye_mask(edge), penalty, 0.0)
                system[down, across] = part
                high_a[down, across], low_a[down, across] = split(part)
                size = jnp.abs(part)
                shifted[down, across] = size.astype(BF16)
                sums[q] = sums[q] + size.reshape(edge // 8, 8, edge).sum(0)
        sums = jnp.concatenate([jnp.broadcast_to(jnp.sum(part, axis=0, keepdims=True), (8, edge)) for part in sums], 1)
        trial = sums.astype(BF16)
        high = jnp.max(dot(trial, shifted[...]) / trial.astype(F32)) * (1.005 / penalty)
        delta = (high - 1.0) / (high + 1.0)
        alpha = 2.0 / ((1.0 + high) * penalty)
        c, later = newton_scale(delta)

        def begin(target, dtype):
            for p, down in enumerate(spans):
                for q, across in enumerate(spans):
                    part = (-c * alpha * alpha) * system[down, across]
                    if p == q:
                        part = part + jnp.where(eye_mask(edge), 2.0 * c * alpha, 0.0)
                    target[down, across] = part.astype(dtype)

        begin(start, BF16)
        hard = jnp.logical_not(high <= EASY)
        lane = lax.broadcasted_iota(jnp.int32, (1, LANES), 1)
        info[...] = jnp.where(lane == 0, later, jnp.where(hard, 1.0, 0.0))

        @pl.when(hard)
        def _():
            begin(inverse, F32)
            careful(later)

    def careful(delta):
        sub = lax.broadcasted_iota(jnp.int32, (8, count), 0)
        mixed = (lax.broadcasted_iota(jnp.int32, (8, count), 1) + 1) * (sub * 40503 + 30011)
        mixed = (mixed ^ (mixed >> 7)) * 9973
        signs = jnp.where(((mixed >> 9) & 1) == 1, 1.0, -1.0)

        def coarse(state):
            step, delta = state
            x = inverse[...].astype(BF16)
            shifted[...] = dot(high_a[...], x).astype(BF16)
            c, later = newton_scale(delta)
            inverse[...] = c * (2.0 * inverse[...] - dot(x, shifted[...]))
            return step + 1, later

        lax.while_loop(lambda state: (state[1] > 0.085) & (state[0] < 12), coarse, (0, delta))

        def polish(state):
            step, _ = state
            high_x[...], low_x[...] = split(inverse[...])
            ah, al, xh, xl = high_a[...], low_a[...], high_x[...], low_x[...]
            shifted[...] = (eye(count) - (dot(ah, xh) + (dot(ah, xl) + dot(al, xh)))).astype(BF16)
            once = signs - thin(thin(signs, xh, xl), ah, al)
            twice = once - thin(thin(once, xh, xl), ah, al)
            inverse[...] = inverse[...] + dot(xh, shifted[...])
            return step + 1, jnp.sum(twice * twice) * (1.0 / 8.0)

        _, worst = lax.while_loop(
            lambda state: jnp.logical_not(state[1] < 0.001) & (state[0] < 8), polish, (0, jnp.float32(1e9))
        )

        @pl.when(jnp.logical_not(worst < 0.001))
        def _():
            invert_by_pivots(system, inverse)

    pl.when(lax.axis_index("feat") == lax.axis_size("feat") - 1)(solve)


def feature_steps(all_s, all_u, phi, high_p, low_p):
    reduced, count = all_s.shape

    def first():
        phi[0:reduced, :] = all_s[...]

    def products(i, row):
        phi[row : row + reduced - i, :] = all_s[i : i + 1, :] * all_s[i:reduced, :]

    def ending(row):
        phi[row : row + 1, :] = all_u[...]
        phi[row + 1 : row + 2, :] = jnp.ones((1, count), F32)
        if row + 2 < phi.shape[0]:
            phi[row + 2 :, :] = jnp.zeros((phi.shape[0] - row - 2, count), F32)

    steps = [first]
    row = reduced
    for i in range(reduced):
        steps.append(functools.partial(products, i, row))
        row += reduced - i
    steps.append(functools.partial(ending, row))

    def narrow(rows):
        high_p[rows, :], low_p[rows, :] = split(phi[rows, :])

    for k in range(0, phi.shape[0], LANES):
        steps.append(functools.partial(narrow, slice(k, k + LANES)))
    return steps


def lanes_of(value):
    return jnp.sum(value.reshape(-1, value.shape[-1]), axis=0, keepdims=True)


def second_kernel(
    all_s, all_u, all_t, high_a, low_a, begin, inverse, info, after, duals, last, history,
    phi, high_p, low_p, high_w, low_w, better, high_b, low_b, gap, answer,
    own1, own2, land1, land2, out1, out2, mean1, mean2, mine, ship, span,
    send1, recv1, spread1, got1, send2, recv2, spread2, got2, ship_send, ship_recv,
    *, width, first_owners, second_owners, order,
):
    slabs = lax.axis_size("slab")
    feats = lax.axis_size("feat")
    me = lax.axis_index("slab")
    core = lax.axis_index("feat")
    owners, reduced, wide = own1.shape
    half = reduced // feats
    count = all_s.shape[1]
    head = feats - 1
    leading = core == head
    everyones = sorted(set(first_owners) | set(second_owners))

    def among(slab_list):
        return functools.reduce(jnp.logical_or, [me == slab for slab in slab_list])

    def place_in(slab_list):
        return functools.reduce(lambda a, b: a + b, [jnp.where(me == slab, k, 0) for k, slab in enumerate(slab_list)])

    inside, inside1, inside2 = among(everyones), among(first_owners), among(second_owners)
    spot1, spot2 = place_in(first_owners), place_in(second_owners)

    def copy(source, target, send, recv, slab, feat):
        return pltpu.make_async_remote_copy(
            src_ref=source, dst_ref=target, send_sem=send, recv_sem=recv,
            device_id={"slab": slab, "feat": feat}, device_id_type=pl.DeviceIdType.MESH,
        )

    def arrived(target, size, sem):
        part = target.at[pl.ds(0, size)]
        copy(part, part, sem, sem, me, core).wait_recv()

    def departed(source, size, sem):
        part = source.at[pl.ds(0, size)]
        copy(part, part, sem, sem, me, core).wait_send()

    def each(order, body):
        if len(order) <= 16:
            for d in order:
                body(d)
            return

        def step(d, carry):
            body(d)
            return carry

        lax.fori_loop(min(order), max(order) + 1, step, 0)

    far = sorted(range(1, slabs), key=lambda d: -min(d, slabs - d))

    def slab_of(d):
        return lax.rem(me + d, slabs)

    def split_on(flag, yes, no):
        pl.when(flag)(yes)
        pl.when(jnp.logical_not(flag))(no)

    barrier = pltpu.get_barrier_semaphore()

    def greet(slab, feat):
        pl.semaphore_signal(
            barrier, inc=1, device_id={"slab": slab, "feat": feat}, device_id_type=pl.DeviceIdType.MESH
        )

    @pl.when(leading & inside)
    def _():
        for f in range(feats):
            each(far, lambda d, f=f: greet(slab_of(d), f))
        for f in range(head):
            greet(me, f)

    @pl.when(jnp.logical_not(leading & inside))
    def _():
        for slab in everyones:
            greet(slab, head)

    @pl.when(leading & jnp.logical_not(inside))
    def _():
        for f in range(head):
            greet(me, f)

    @pl.when(jnp.logical_not(leading) & jnp.logical_not(inside))
    def _():
        greet(me, head)

    def scatter(source, landing, send, recv, slab_list, group):
        for k, slab in enumerate(slab_list):
            if k not in group:
                continue

            @pl.when(me != slab)
            def _():
                copy(source.at[k], landing.at[me], send, recv, slab, head).start()

    def joined(buffer, rows):
        return jnp.concatenate([buffer[k][:rows] for k in range(owners)], 1)

    def owner_first():
        land1[me] = own1[spot1]
        arrived(land1, slabs - 1, recv1)
        out1[...] = land1[...].sum(0) * (1.0 / slabs)
        each(far, lambda d: copy(out1, mean1.at[spot1], spread1, got1, slab_of(d), head).start())
        mean1[spot1] = out1[...]

    def owner_second():
        old = mean1[spot2]
        dual1 = lanes_of(jnp.square(old))
        land2[me] = own2[spot2]
        arrived(land2, slabs - 1, recv2)
        whole = land2[...].sum(0)
        new = whole[:reduced] * (1.0 / slabs)
        primal2 = lanes_of(jnp.square(land2[:, 0:reduced] - new[None]))
        dual2 = lanes_of(jnp.square(new - old))
        scale = slabs * penalty * penalty
        stats = jnp.concatenate([whole[reduced : reduced + 1], primal2, dual1 * scale, dual2 * scale], 0)
        for f in range(feats):
            out2[f, 0:half] = new[f * half : (f + 1) * half]
            out2[f, half : half + 4] = stats

        def one(slab):
            for f in range(feats):

                @pl.when((me != slab) | (f != head))
                def _():
                    copy(out2.at[f], mean2.at[spot2], spread2, got2, slab, f).start()

        for slab in order:
            one(slab)
        mean2[spot2] = out2[head]

    near_half = -(-owners // 3)
    groups = [range(k, min(k + near_half, owners)) for k in range(0, owners, near_half)]

    def leader():
        ah, al = high_a[...], low_a[...]
        delta = info[0:1, 0:1]
        kept = info[0:1, 1:2] > 0.5
        middle = up(count // 2, LANES)
        parts = (slice(0, middle), slice(middle, count))
        steps = feature_steps(all_s, all_u, phi, high_p, low_p)
        chunk = -(-len(steps) // (2 * STEPS))
        old, fresh, spare = begin, high_b, low_b
        size = jnp.ones((1, 1), F32)
        for step in range(STEPS):
            c, delta = newton_scale(delta)
            for part in parts:
                gap[:, part] = dot(ah, old[:, part]).astype(BF16)
                for _ in range(min(chunk, len(steps))):
                    steps.pop(0)()
            x = old[...]
            for part in parts:
                value = (2.0 / size) * old[:, part].astype(F32) - dot(x, gap[:, part])
                if step == STEPS - 1:
                    value = value * (c * size * size)
                fresh[:, part] = value.astype(BF16)
            size = c * size * size
            old, fresh, spare = fresh, spare, fresh
        b = all_t[...] * (1.0 / count)
        x = old[...]
        for part in parts:
            less_eye(dot(ah, x[:, part]) + dot(al, x[:, part]), gap, part)
        c, _ = newton_scale(delta)
        for part in parts:
            value = c * (x[:, part].astype(F32) - dot(x, gap[:, part]))
            better[:, part] = jnp.where(kept, inverse[:, part], value)
        high_b[...], low_b[...] = split(better[...])
        xh, xl = high_b[...], low_b[...]
        y = thin(b, xh, xl)
        y = y + thin(b - thin(y, ah, al), xh, xl)
        y = y + thin(b - thin(y, ah, al), xh, xl)
        answer[...] = y
        for group in groups:
            across = slice(group.start * wide, group.stop * wide)
            start_value = thin(y, high_p[across, :], low_p[across, :], NT)
            for k in group:
                near = (k - group.start) * wide
                own1[k] = start_value[:, near : near + wide]
            if group is groups[0]:
                split_on(
                    inside,
                    lambda: pl.semaphore_wait(barrier, slabs * feats - 1),
                    lambda: pl.semaphore_wait(barrier, len(everyones) + feats - 1),
                )
            scatter(own1, land1, send1, recv1, first_owners, group)

        for _ in range(2):
            bh, bl = high_b[...], low_b[...]
            for part in parts:
                less_eye(dot(ah, bh[:, part]) + (dot(ah, bl[:, part]) + dot(al, bh[:, part])), gap, part)
            for part in parts:
                better[:, part] = better[:, part] - dot(bh, gap[:, part])
            high_b[...], low_b[...] = split(better[...])
        pl.when(inside1)(owner_first)
        weights = dot(high_b[...], high_p[...], NT) + (
            dot(high_b[...], low_p[...], NT) + dot(low_b[...], high_p[...], NT)
        )
        high_w[...], low_w[...] = split(weights)

        split_on(
            inside1,
            lambda: arrived(mean1, owners - 1, got1),
            lambda: arrived(mean1, owners, got1),
        )
        first = joined(own1, reduced)
        mean = joined(mean1, reduced)
        v = thin(mean, high_p[...], low_p[...]) * (2.0 / (count * penalty)) + answer[...]
        primal1 = jnp.sum(jnp.square(first - mean), axis=0, keepdims=True)
        results = []
        for group in groups:
            across = slice(group.start * wide, group.stop * wide)
            result = first[:, across] + 2.0 * mean[:, across] - thin(v, high_w[:, across], low_w[:, across])
            for k in group:
                near = (k - group.start) * wide
                own2[k, 0:reduced] = result[:, near : near + wide]
                own2[k, reduced : reduced + 1] = primal1[:, k * wide : (k + 1) * wide]
            scatter(own2, land2, send2, recv2, second_owners, group)
            results.append(result)
        result = jnp.concatenate(results, 1)
        change = (first - mean) + result
        for f in range(head):
            ship[f, 0] = result[f * half : (f + 1) * half]
            ship[f, 1] = change[f * half : (f + 1) * half]
            copy(ship.at[f], mine, ship_send.at[f], ship_recv, me, f).start()
        mine[0] = result[head * half :]
        mine[1] = change[head * half :]
        pl.when(inside2)(owner_second)

        split_on(inside1, lambda: departed(own1, owners - 1, send1), lambda: departed(own1, owners, send1))
        split_on(inside2, lambda: departed(own2, owners - 1, send2), lambda: departed(own2, owners, send2))
        for f in range(head):
            copy(ship.at[f], mine, ship_send.at[f], ship_recv, me, core).wait_send()

    def follower():
        split_on(
            inside,
            lambda: pl.semaphore_wait(barrier, len(everyones)),
            lambda: pl.semaphore_wait(barrier, len(everyones) + 1),
        )
        copy(ship.at[0], mine, ship_send.at[0], ship_recv, me, core).wait_recv()

    split_on(leading, leader, follower)
    split_on(
        leading & inside2,
        lambda: arrived(mean2, owners - 1, got2),
        lambda: arrived(mean2, owners, got2),
    )
    new = joined(mean2, half)
    after[...] = mine[0]
    last[...] = new
    duals[...] = mine[1] - new
    sums = mean2[0][half : half + 4]
    for k in range(1, owners):
        sums = sums + mean2[k][half : half + 4]
    sums = jnp.sum(sums, axis=1, keepdims=True)
    history[...] = jnp.broadcast_to(jnp.sqrt(sums * (1.0 / (slabs * reduced * width))), history.shape)

    @pl.when(leading & inside1)
    def _():
        departed(land1, slabs - 1, spread1)

    @pl.when(leading & inside2)
    def _():
        departed(span, slabs * feats - 1, spread2)


def last_kernel(after, duals, last, history, out_after, out_duals, out_last, out_history):
    half, width = out_last.shape
    for r in range(half):
        out_after[r] = after[r : r + 1, :width]
        out_duals[r] = duals[r : r + 1, :width]
    out_last[...] = last[:, :width]
    for r in range(2):
        out_history[r : r + 1, :] = jnp.concatenate([history[2 * r + k : 2 * r + k + 1, 0:1] for k in range(2)], 1)


def shards(states, inputs, targets, *, spots):
    reduced, own = states.shape
    feats = lax.axis_size("feat")
    slabs = lax.axis_size("slab")
    half = reduced // feats
    width = reduced + reduced * (reduced + 1) // 2 + 2
    count = own * feats
    tiles = up(width, LANES) // LANES
    wide = -(-tiles // slabs) * LANES
    columns = up(width, wide)
    owners = columns // wide
    vmem = pl.BlockSpec(memory_space=pltpu.VMEM)
    dma = pltpu.SemaphoreType.DMA

    def shape(*sizes, dtype=F32):
        return jax.ShapeDtypeStruct(sizes, dtype)

    def hold(*sizes, dtype=F32):
        return pltpu.VMEM(sizes, dtype)

    gathered = pl.pallas_call(
        exchange_kernel,
        out_shape=(shape(reduced, count), shape(1, count), shape(reduced, count)),
        in_specs=[pl.BlockSpec(memory_space=pltpu.HBM)] * 3,
        out_specs=(vmem,) * 3,
        scratch_shapes=[dma((3,)), dma((3,)), dma((feats, 3))],
        compiler_params=pltpu.CompilerParams(vmem_limit_bytes=LIMIT, collective_id=1, has_side_effects=True),
        name="exchange",
    )(*[pltpu.with_memory_space_constraint(x, pltpu.HBM) for x in (states, inputs[None], targets)])
    square = shape(count, count)
    short = shape(count, count, dtype=BF16)
    solved = pl.pallas_call(
        inverse_kernel,
        out_shape=(short, short, short, square, shape(1, LANES)),
        in_specs=[vmem] * 2,
        out_specs=(vmem,) * 5,
        scratch_shapes=[
            hold(count, count), hold(count, count, dtype=BF16),
            hold(count, count, dtype=BF16), hold(count, count, dtype=BF16),
        ],
        compiler_params=pltpu.CompilerParams(vmem_limit_bytes=LIMIT),
        name="local_inverse",
    )(gathered[0], gathered[1])
    block = shape(half, columns)
    first_owners, second_owners, order = choose(spots, owners)
    after, duals, last, history = pl.pallas_call(
        functools.partial(
            second_kernel, width=width, first_owners=first_owners, second_owners=second_owners, order=order
        ),
        out_shape=(block, block, block, shape(4, LANES)),
        in_specs=[vmem] * 8,
        out_specs=(vmem,) * 4,
        scratch_shapes=[
            hold(columns, count),
            hold(columns, count, dtype=BF16), hold(columns, count, dtype=BF16),
            hold(count, columns, dtype=BF16), hold(count, columns, dtype=BF16),
            hold(count, count), hold(count, count, dtype=BF16), hold(count, count, dtype=BF16),
            hold(count, count, dtype=BF16), hold(reduced, count),
            hold(owners, reduced, wide), hold(owners, reduced + 1, wide),
            hold(slabs, reduced, wide), hold(slabs, reduced + 1, wide),
            hold(reduced, wide), hold(feats, half + 4, wide),
            hold(owners, reduced, wide), hold(owners, half + 4, wide),
            hold(2, half, columns), hold(max(feats - 1, 1), 2, half, columns),
            hold(slabs * feats, half + 4, wide),
            dma, dma, dma, dma, dma, dma, dma, dma, dma((max(feats - 1, 1),)), dma,
        ],
        compiler_params=pltpu.CompilerParams(vmem_limit_bytes=2 * LIMIT, collective_id=0, has_side_effects=True),
        name="second_and_averages",
    )(*gathered, *solved)
    shard = shape(half, width)
    spread_rows = shape(half, 1, width)
    after, duals, last, history = pl.pallas_call(
        last_kernel,
        out_shape=(spread_rows, spread_rows, shard, shape(2, 2)),
        in_specs=[vmem] * 4,
        out_specs=(vmem,) * 4,
        compiler_params=pltpu.CompilerParams(vmem_limit_bytes=4 * 2**20),
        name="outputs",
    )(after, duals, last, history)
    return (jnp.swapaxes(after, 0, 1), jnp.swapaxes(duals, 0, 1), last, history)


def choose(spots, owners):
    slabs = range(len(spots))
    apart = [[sum(abs(a - b) for a, b in zip(spots[p], spots[q])) for q in slabs] for p in slabs]
    first = sorted(slabs, key=lambda q: (max(apart[q]), -apart[0][q], q))[:owners]
    second = sorted(slabs, key=lambda q: (max(apart[q]), apart[0][q], q))[:owners]
    return sorted(first), sorted(second, reverse=True), sorted(slabs, key=lambda p: (apart[0][p], p))


def solution(mesh):
    spots = [
        tuple(getattr(device, "coords", None) or (index,)) for index, device in enumerate(mesh.devices[:, 0])
    ]
    in_specs = (P(None, ("slab", "feat")), P(("slab", "feat")), P(None, ("slab", "feat")))
    out_specs = (P("slab", "feat", None), P("slab", "feat", None), P("feat", None), P())
    body = functools.partial(shards, spots=spots)
    return jax.shard_map(body, mesh=mesh, in_specs=in_specs, out_specs=out_specs, check_vma=False)
```
